32 devices in a mesh: dp: 8 (over z, x), cent: 4 (over y, core).
Axes of the slice: x: 2, y: 2, z: 4, core: 2. Of those that a mesh axis runs over, the one named last changes fastest.
Arguments:
- documents: bfloat16 [16384, 2048], P(('dp', 'cent')), may hold values from -6 to 6
- assigned: int32 [16384], P(('dp', 'cent')), may hold values from 0 to 12287, as said below
- centroids: bfloat16 [12288, 2048], P(('dp', 'cent')), may hold values from -6 to 6
- owner_slot: int32 [12288], replicated, may hold values from 0 to 12287, as said below
Outputs:
- prototypicality: float32 [16384], P(('dp', 'cent'))
- redundancy: float32 [16384], P(('dp', 'cent'))
- cluster_stats: float32 [3, 12288], P(None, ('dp', 'cent'))
The draws below stay inside these ranges and needn't reach their ends.
Inputs may be any that keep to these rules, and one draw needn't show every extreme that they name: `owner_slot`: A permutation of the cluster numbers. `assigned`: of the 512 documents of one device, at most 32 have a slot in any one owner's block of 384 slots, and at most 80 have slots with the owners that share one dp index; in every draw some device reaches 80, and one owner receives exactly 32 from every device.
All inputs are finite; a program needn't handle non-finite values.
Results may differ from the reference program's by a relative error of at most 0.0003.
Values may be sent and summed in bfloat16 or wider, within the bound.
No kernel may reach another device: no remote copies, remote signals or barrier semaphores. Data moves between devices by JAX's collectives and lax.ppermute only.
A program may use at most 64 MiB of HBM per device.

```python
import jax
import jax.numpy as jnp
from jax import lax

D = 2048
DOC_DEV = 512
CL_DEV = 384
DOCS = 16384
CLUSTERS = 12288
CAP = 32
GCAP = 80
N_CENT = 4
DEVICES = 32


def slot_permutation(key):
    return jax.random.permutation(jax.random.fold_in(key, 11), CLUSTERS).astype(jnp.int32)


def draw_owner_slot(key, part):
    return slot_permutation(key)


def draw_assigned(key, part):
    permuted = slot_permutation(key)
    inverse = jnp.zeros((CLUSTERS,), jnp.int32).at[permuted].set(jnp.arange(CLUSTERS, dtype=jnp.int32))
    base = jax.random.fold_in(key, 23)
    key_forced = jax.random.fold_in(base, 1)
    key_favour = jax.random.fold_in(base, 2)
    key_ticket = jax.random.fold_in(base, 3)
    key_choose = jax.random.fold_in(base, 4)
    key_shuffle = jax.random.fold_in(base, 5)
    key_local = jax.random.fold_in(base, 6)
    row_count = DEVICES // N_CENT
    per_row = N_CENT * CAP
    forced = jax.random.randint(key_forced, (), 0, DEVICES, dtype=jnp.int32)
    forced_row = forced // N_CENT
    forced_col = forced % N_CENT
    row_ids = jnp.arange(row_count, dtype=jnp.int32)[None, :]
    favour = jax.random.randint(key_favour, (DEVICES, row_count), 0, N_CENT, dtype=jnp.int32)
    favour = jnp.where(row_ids == forced_row, forced_col, favour)
    ticket_ids = jnp.arange(per_row, dtype=jnp.int32)
    ticket_col = ticket_ids // CAP
    noise = jax.random.randint(key_ticket, (DEVICES, row_count, per_row), 0, 1 << 19, dtype=jnp.int32)
    boost = jnp.where(ticket_col[None, None, :] == favour[:, :, None], 1 << 29, 0).astype(jnp.int32)
    score = noise * per_row + ticket_ids[None, None, :] + boost
    kept = jnp.argsort(-score, axis=-1)[:, :, :GCAP].astype(jnp.int32)
    kept_owner = row_ids[:, :, None] * N_CENT + kept // CAP
    kept_owner = kept_owner.reshape(DEVICES, row_count * GCAP)
    pool = row_count * GCAP
    pool_ids = jnp.arange(pool, dtype=jnp.int32)
    pool_row = pool_ids // GCAP
    noise_two = jax.random.randint(key_choose, (DEVICES, pool), 0, 1 << 19, dtype=jnp.int32)
    boost_two = jnp.where(pool_row == forced_row, 1 << 29, 0).astype(jnp.int32)
    score_two = noise_two * pool + pool_ids[None, :] + boost_two[None, :]
    chosen = jnp.argsort(-score_two, axis=-1)[:, :DOC_DEV].astype(jnp.int32)
    chosen_owner = jnp.take_along_axis(kept_owner, chosen, axis=1)
    noise_three = jax.random.randint(key_shuffle, (DEVICES, DOC_DEV), 0, 1 << 19, dtype=jnp.int32)
    score_three = noise_three * DOC_DEV + jnp.arange(DOC_DEV, dtype=jnp.int32)[None, :]
    shuffled = jnp.argsort(score_three, axis=-1).astype(jnp.int32)
    final_owner = jnp.take_along_axis(chosen_owner, shuffled, axis=1)
    local_draws = jax.random.randint(key_local, (3, DEVICES, DOC_DEV), 0, CL_DEV, dtype=jnp.int32)
    local_ids = jnp.min(local_draws, axis=0)
    slot_ids = final_owner * CL_DEV + local_ids
    return inverse[slot_ids.reshape(DOCS)]


def block_levels(stream_key, extent, pieces, smallest, high):
    gain, own = 1.0, jax.random.fold_in(stream_key, 6)
    for dim, shards_of in pieces:
        steps = jnp.exp(jax.random.uniform(jax.random.fold_in(own, dim), (shards_of,), jnp.float32, smallest / len(pieces), high / len(pieces)))
        gain = gain * jnp.repeat(steps, extent[dim] // shards_of).reshape([-1 if axis == dim else 1 for axis in range(len(extent))])
    return gain


def normal_values(key, shape, scale, reach, cuts=(), held_as=jnp.bfloat16):
    entries = jax.random.normal(key, shape, jnp.float32) * scale
    if len(cuts) > 0:
        entries = block_levels(key, shape, cuts, -0.22, 0.18) * entries
    return jnp.clip(entries, min=-reach, max=reach).astype(held_as)


def setup_inputs(seed: int = 0) -> dict:
    key_list = jax.random.split(jax.random.key(seed), 5)
    documents = normal_values(key_list[0], (DOCS, D), 1.0, 6.0, ((0, 32),))
    assigned = draw_assigned(jax.random.fold_in(key_list[4], 71), 0)
    centroids = normal_values(key_list[2], (CLUSTERS, D), 1.0, 6.0, ((0, 32),))
    owner_slot = draw_owner_slot(jax.random.fold_in(key_list[4], 71), 0)
    return dict(documents=documents, assigned=assigned, centroids=centroids, owner_slot=owner_slot)


def reference(documents, assigned, centroids, owner_slot):
    slot_ids = owner_slot[assigned]
    owner_ids = slot_ids // CL_DEV
    cent_sq = lax.optimization_barrier(jnp.sum(jnp.square(centroids.astype(jnp.float32)), axis=1))

    def block_sim(packed):
        doc_block, slot_block = packed
        doc_rows = doc_block.astype(jnp.float32)
        cent_rows = centroids[slot_block].astype(jnp.float32)
        cross_dot = lax.optimization_barrier(jnp.sum(doc_rows * cent_rows, axis=1))
        self_sq = lax.optimization_barrier(jnp.sum(doc_rows * doc_rows, axis=1))
        similar = cross_dot * lax.rsqrt(self_sq + 1.0) * lax.rsqrt(cent_sq[slot_block] + 1.0)
        return (similar, self_sq)
    similarity, self_sq = lax.map(block_sim, (documents.reshape(DEVICES, DOC_DEV, D), slot_ids.reshape(DEVICES, DOC_DEV)))
    similarity = similarity.reshape(DOCS)
    self_sq = self_sq.reshape(DOCS)
    counts = jax.ops.segment_sum(jnp.ones((DOCS,), jnp.float32), slot_ids, num_segments=CLUSTERS)
    totals = jax.ops.segment_sum(similarity, slot_ids, num_segments=CLUSTERS)
    squares = jax.ops.segment_sum(similarity * similarity, slot_ids, num_segments=CLUSTERS)
    cluster_stats = jnp.stack([counts, totals, squares])
    count_floor = jnp.maximum(counts, 1.0)
    mean_sim = totals / count_floor
    variance = jnp.maximum(squares / count_floor - mean_sim * mean_sim, 0.0)
    prototypicality = (mean_sim[slot_ids] - similarity) / jnp.sqrt(variance[slot_ids] + 1.0 / D)
    owner_grid = owner_ids.reshape(DEVICES, DOC_DEV)
    is_owner = (owner_grid[:, :, None] == jnp.arange(DEVICES, dtype=jnp.int32)[None, None, :]).astype(jnp.int32)
    rank_ids = lax.optimization_barrier(jnp.sum((jnp.cumsum(is_owner, axis=1) - 1) * is_owner, axis=2)).astype(jnp.int32)
    source_ids = jnp.arange(DEVICES, dtype=jnp.int32)[:, None]
    position = owner_grid * (DEVICES * CAP) + source_ids * CAP + rank_ids
    member_table = jnp.full((DEVICES * DEVICES * CAP,), DOCS, jnp.int32)
    member_table = member_table.at[position.reshape(-1)].set(jnp.arange(DOCS, dtype=jnp.int32))
    member_table = member_table.reshape(DEVICES, DEVICES * CAP)
    inverse_norm = lax.rsqrt(self_sq + 1.0)
    slot_count = DEVICES * CAP
    not_self = jnp.arange(slot_count, dtype=jnp.int32)[:, None] != jnp.arange(slot_count, dtype=jnp.int32)[None, :]

    def owner_redundancy(members):
        is_live = members < DOCS
        safe_ids = jnp.minimum(members, DOCS - 1)
        doc_rows = documents[safe_ids].astype(jnp.float32)
        gram_block = jnp.dot(doc_rows, doc_rows.T, precision=lax.Precision.HIGHEST)
        row_scale = jnp.where(is_live, inverse_norm[safe_ids], 0.0)
        cosine = gram_block * row_scale[:, None] * row_scale[None, :]
        cluster_tag = jnp.where(is_live, slot_ids[safe_ids], -1)
        same_cluster = (cluster_tag[:, None] == cluster_tag[None, :]) & is_live[:, None] & not_self
        return jnp.sqrt(jnp.float32(D)) * lax.optimization_barrier(jnp.max(jnp.where(same_cluster, cosine, 0.0), axis=1))
    redundant = lax.map(owner_redundancy, member_table)
    redundancy = jnp.zeros((DOCS,), jnp.float32).at[member_table.reshape(-1)].set(redundant.reshape(-1), mode='drop')
    return (prototypicality, redundancy, cluster_stats)
```

```python
import math

import jax
import jax.numpy as jnp
from jax import lax
from jax.experimental import pallas as pl
from jax.experimental.pallas import tpu as pltpu
from jax.sharding import PartitionSpec as P

LANES = 128
HIGHEST = lax.Precision.HIGHEST


def bucket_positions(target, groups, capacity):
    length = target.shape[0]
    indicator = (target[:, None] == jnp.arange(groups, dtype=jnp.int32)[None, :]).astype(
        jnp.bfloat16
    )
    earlier = (
        lax.broadcasted_iota(jnp.int32, (length, length), 0)
        > lax.broadcasted_iota(jnp.int32, (length, length), 1)
    ).astype(jnp.bfloat16)
    before = jnp.dot(earlier, indicator, preferred_element_type=jnp.float32)
    rank_ids = jnp.sum(before * indicator.astype(jnp.float32), axis=1).astype(jnp.int32)
    return jnp.where(target < groups, target * capacity + rank_ids, groups * capacity)


def owner_work(incoming, incoming_tags, centroids):
    table_rows = centroids.shape[0]
    width = incoming.shape[1]
    length = incoming_tags.shape[0]
    is_live = incoming_tags >= 0
    safe_slot = jnp.clip(incoming_tags, 0, table_rows - 1)
    cent_sq = jnp.einsum("kd,kd->k", centroids, centroids, preferred_element_type=jnp.float32)
    cent_vec = centroids[safe_slot]
    cross_dot = jnp.einsum("sd,sd->s", incoming, cent_vec, preferred_element_type=jnp.float32)
    self_sq = jnp.einsum("sd,sd->s", incoming, incoming, preferred_element_type=jnp.float32)
    inverse_norm = lax.rsqrt(self_sq + 1.0)
    similarity = cross_dot * inverse_norm * lax.rsqrt(cent_sq[safe_slot] + 1.0)
    members = (incoming_tags[:, None] == jnp.arange(table_rows, dtype=jnp.int32)[None, :]).astype(
        jnp.float32
    )
    live_weight = is_live.astype(jnp.float32)
    moments = jnp.stack(
        [live_weight, live_weight * similarity, live_weight * similarity * similarity]
    )
    cluster_totals = jnp.dot(
        moments, members, precision=lax.Precision.HIGHEST, preferred_element_type=jnp.float32
    )
    count_floor = jnp.maximum(cluster_totals[0], 1.0)
    mean_sim = cluster_totals[1] / count_floor
    variance = jnp.maximum(cluster_totals[2] / count_floor - mean_sim * mean_sim, 0.0)
    proto_score = jnp.where(
        is_live,
        (mean_sim[safe_slot] - similarity) / jnp.sqrt(variance[safe_slot] + 1.0 / width),
        0.0,
    )
    gram_block = lax.dot_general(
        incoming, incoming, (((1,), (1,)), ((), ())), preferred_element_type=jnp.float32
    )
    cosine = gram_block * inverse_norm[:, None] * inverse_norm[None, :]
    not_self = lax.broadcasted_iota(jnp.int32, (length, length), 0) != lax.broadcasted_iota(
        jnp.int32, (length, length), 1
    )
    same_cluster = (incoming_tags[:, None] == incoming_tags[None, :]) & is_live[:, None] & not_self
    redundant = math.sqrt(width) * jnp.max(jnp.where(same_cluster, cosine, 0.0), axis=1)
    return (cluster_totals, proto_score, redundant)


def iota(shape, dim):
    return lax.broadcasted_iota(jnp.int32, shape, dim)


def mm(a, b, dims, precision=None):
    return lax.dot_general(
        a, b, (dims, ((), ())), precision=precision, preferred_element_type=jnp.float32
    )


def device_index(cent_count):
    return lax.axis_index("dp") * cent_count + lax.axis_index("cent")


def vmem(count):
    return [pl.BlockSpec(memory_space=pltpu.VMEM)] * count


def params():
    return pltpu.CompilerParams(vmem_limit_bytes=56 * 1024 * 1024)


def local(documents, assigned, centroids, owner_slot):
    docs, width = documents.shape
    rows = centroids.shape[0]
    dp = lax.axis_size("dp")
    cent = lax.axis_size("cent")
    owners = dp * cent
    cap = 2 * docs // owners
    row_cap = 5 * cent * cap // 8
    group = cent * cap
    near = dp // 2
    clusters = owner_slot.shape[0]
    wide = width + LANES
    root = math.sqrt(width)

    def route(assigned_ref, table_ref, docs_ref, *outs):
        far_refs = outs[:near]
        tag_refs = outs[near : 2 * near]
        key_ref = outs[2 * near]
        me = device_index(cent)
        a = assigned_ref[...]
        pick = (iota((clusters // LANES, docs), 0) == a // LANES).astype(jnp.float32)
        lines = mm(table_ref[...].astype(jnp.float32), pick, ((0,), (0,)), HIGHEST)
        slot = jnp.sum(
            jnp.where(iota((LANES, docs), 0) == a % LANES, lines, 0.0), axis=0, keepdims=True
        )
        owner = jnp.floor((slot + 0.5) * (1.0 / rows))
        home = (slot - owner * rows).astype(jnp.int32) + 1
        rel = owner.astype(jnp.int32) ^ me
        which = iota((owners, docs), 0)
        mine = which == rel
        earlier = (iota((docs, docs), 0) < iota((docs, docs), 1)).astype(jnp.bfloat16)
        before = mm(mine.astype(jnp.bfloat16), earlier, ((1,), (0,)))
        rank = jnp.sum(jnp.where(mine, before, 0.0), axis=0, keepdims=True).astype(jnp.int32)
        row_rank = jnp.sum(
            jnp.where(which // cent == rel // cent, before, 0.0), axis=0, keepdims=True
        ).astype(jnp.int32)
        key = rel * cap + rank
        row_key = (rel // cent) * row_cap + row_rank
        inner = key % group
        key_ref[0:1, :] = key
        key_ref[1:2, :] = home
        sub = iota((8, docs), 0)
        facts = jnp.where(sub == 0, inner, jnp.where(sub == 1, home, 0)).astype(jnp.float32)
        for m in range(near):
            sel = iota((row_cap, docs), 0) + (near + m) * row_cap == row_key
            picked = mm(sel.astype(jnp.bfloat16), docs_ref[...], ((1,), (0,)))
            far_refs[m][...] = picked.astype(jnp.bfloat16)
            tags = mm(facts, sel.astype(jnp.float32), ((1,), (1,)), HIGHEST)
            tag_refs[m][...] = jnp.zeros((8, LANES), jnp.int32)
            tag_refs[m][:, :row_cap] = tags.astype(jnp.int32)

    def emit(sel, marks, data, outs):
        picked = mm(sel.astype(jnp.bfloat16), data, ((1,), (0,))).astype(jnp.bfloat16)
        mark = jnp.sum(jnp.where(sel, marks, 0), axis=1, keepdims=True)
        ext = jnp.where(iota((group, LANES), 1) < LANES // 2, mark % LANES, mark // LANES)
        ext = ext.astype(jnp.float32).astype(jnp.bfloat16)
        for e in range(cent):
            outs[e][:, :width] = picked[e * cap : (e + 1) * cap]
            outs[e][:, width:] = ext[e * cap : (e + 1) * cap]

    def pack(key_ref, docs_ref, *outs):
        for m in range(near):
            sel = iota((group, docs), 0) + m * group == key_ref[0:1, :]
            emit(sel, key_ref[1:2, :], docs_ref[...], outs[m * cent : (m + 1) * cent])

    def relay(data_ref, tag_ref, *outs):
        marks = tag_ref[1:2, :row_cap]
        sel = (iota((group, row_cap), 0) == tag_ref[0:1, :row_cap]) & (marks > 0)
        emit(sel, marks, data_ref[...], outs)

    total = owners * cap

    def owner_work(*refs):
        blocks = refs[:owners]
        cent_ref, score_ref, stat_ref, x, g, tagc, simc, line = refs[owners:]
        me = device_index(cent)
        for b in range(owners):
            at = pl.ds(b * cap, cap)
            x[at, :] = blocks[b][:, :width]
            ext = blocks[b][:, width:].astype(jnp.float32)
            tagc[at, :] = ext[:, :1] + LANES * ext[:, LANES // 2 : LANES // 2 + 1]
        eye_c = iota((rows, rows), 0) == iota((rows, rows), 1)
        cc = mm(cent_ref[...], cent_ref[...], ((1,), (1,)))
        cent_inv = lax.rsqrt(jnp.sum(jnp.where(eye_c, cc, 0.0), axis=0, keepdims=True) + 1.0)
        eye = iota((group, group), 0) == iota((group, group), 1)

        def to_row(col):
            return jnp.sum(jnp.where(eye, col, 0.0), axis=0, keepdims=True)

        def member(tag):
            return (iota((group, rows), 1) + 1).astype(jnp.float32) == tag

        def first(r, sums):
            at = pl.ds(pl.multiple_of(r * group, group), group)
            xb = x[at, :]
            g[at, :] = mm(xb, x[...], ((1,), (1,)))
            diag = jnp.where(eye, g[at, at], 0.0)
            inv = lax.rsqrt(jnp.sum(diag, axis=1, keepdims=True) + 1.0)
            tag = tagc[at, :]
            line[0:1, at] = to_row(tag)
            line[1:2, at] = lax.rsqrt(jnp.sum(diag, axis=0, keepdims=True) + 1.0)
            own = member(tag)
            cross = mm(xb, cent_ref[...], ((1,), (1,)))
            sim = jnp.sum(jnp.where(own, cross * cent_inv, 0.0), axis=1, keepdims=True) * inv
            simc[at, 0:1] = sim
            simc[at, 1:2] = inv
            return (
                sums[0] + jnp.sum(own.astype(jnp.float32), axis=0, keepdims=True),
                sums[1] + jnp.sum(jnp.where(own, sim, 0.0), axis=0, keepdims=True),
                sums[2] + jnp.sum(jnp.where(own, sim * sim, 0.0), axis=0, keepdims=True),
            )

        zero = jnp.zeros((1, rows), jnp.float32)
        count, s1, s2 = lax.fori_loop(0, dp, first, (zero, zero, zero))
        stat_ref[0:1, :] = count
        stat_ref[1:2, :] = s1
        stat_ref[2:3, :] = s2
        floor = jnp.maximum(count, 1.0)
        mean = s1 / floor
        var = jnp.maximum(s2 / floor - mean * mean, 0.0)
        spread = 1.0 / jnp.sqrt(var + 1.0 / width)

        def second(r, carry):
            at = pl.ds(pl.multiple_of(r * group, group), group)
            tag = tagc[at, :]
            same = (tag == line[0:1, :]) & (
                iota((group, total), 0) + r * group != iota((group, total), 1)
            )
            best = jnp.max(jnp.where(same, g[at, :] * line[1:2, :], 0.0), axis=1, keepdims=True)
            red = best * simc[at, 1:2] * root
            own = member(tag)
            mean_d = jnp.sum(jnp.where(own, mean, 0.0), axis=1, keepdims=True)
            spread_d = jnp.sum(jnp.where(own, spread, 0.0), axis=1, keepdims=True)
            score = to_row((mean_d - simc[at, 0:1]) * spread_d)
            red = to_row(red)
            for e in range(cent):
                part = slice(e * cap, (e + 1) * cap)
                score_ref[pl.ds((r * cent + e) ^ me, 1), :] = jnp.concatenate(
                    [score[:, part], red[:, part]], axis=1
                )
            return carry

        lax.fori_loop(0, dp, second, 0)

    def unpack(score_ref, key_ref, out_ref, red_ref):
        me = device_index(cent)
        key = key_ref[0:1, :]
        pick = (iota((owners, docs), 0) == (key // cap) ^ me).astype(jnp.float32)
        got = mm(score_ref[...], pick, ((0,), (0,)), HIGHEST)
        rank = iota((2 * cap, docs), 0)
        out_ref[...] = jnp.sum(jnp.where(rank == key % cap, got, 0.0), axis=0, keepdims=True)
        red_ref[...] = jnp.sum(jnp.where(rank == key % cap + cap, got, 0.0), axis=0, keepdims=True)

    f32 = lambda *s: jax.ShapeDtypeStruct(s, jnp.float32)
    bf16 = lambda *s: jax.ShapeDtypeStruct(s, jnp.bfloat16)
    i32 = lambda *s: jax.ShapeDtypeStruct(s, jnp.int32)
    cost = lambda n: pl.CostEstimate(flops=n, bytes_accessed=1 << 20, transcendentals=0)

    def call(body, ins, outs, name, flops, scratch=()):
        return pl.pallas_call(
            body,
            out_shape=outs,
            in_specs=vmem(len(ins)),
            out_specs=vmem(len(outs)),
            scratch_shapes=list(scratch),
            compiler_params=params(),
            name=name,
            cost_estimate=cost(flops),
        )(*ins)

    def over(axis, size, mask, value):
        return lax.ppermute(value, axis, [(i, i ^ mask) for i in range(size)])

    got = call(
        route,
        (assigned.reshape(1, docs), owner_slot.reshape(-1, LANES), documents),
        [bf16(row_cap, width)] * near + [i32(8, LANES)] * near + [i32(8, docs)],
        "route",
        2 * near * row_cap * docs * width,
    )
    far, tags, key = got[:near], got[near : 2 * near], got[2 * near]
    far_tags = [over("dp", dp, near + m, tags[m]) for m in range(near)]
    far_docs = [over("dp", dp, near + m, far[m]) for m in range(near)]
    sent = call(
        pack,
        (key, documents),
        [bf16(cap, wide)] * (near * cent),
        "pack",
        2 * near * group * docs * width,
    )
    blocks = []
    for m in range(near):
        for e in range(cent):
            block = sent[m * cent + e]
            if m and e:
                pairs = [
                    (i * cent + j, (i ^ m) * cent + (j ^ e)) for i in range(dp) for j in range(cent)
                ]
                block = lax.ppermute(block, ("dp", "cent"), pairs)
            elif m:
                block = over("dp", dp, m, block)
            elif e:
                block = over("cent", cent, e, block)
            blocks.append(block)
    for m in range(near):
        hop = call(
            relay,
            (far_docs[m], far_tags[m]),
            [bf16(cap, wide)] * cent,
            "relay",
            2 * group * row_cap * width,
        )
        blocks += [hop[0]] + [over("cent", cent, e, hop[e]) for e in range(1, cent)]
    scores, stats = call(
        owner_work,
        (*blocks, centroids),
        [f32(owners, 2 * cap), f32(3, rows)],
        "owner",
        2 * total * (total + rows) * width,
        [
            pltpu.VMEM((total, width), jnp.bfloat16),
            pltpu.VMEM((total, total), jnp.float32),
            pltpu.VMEM((total, 1), jnp.float32),
            pltpu.VMEM((total, 2), jnp.float32),
            pltpu.VMEM((8, total), jnp.float32),
        ],
    )
    back = lax.all_to_all(scores, ("dp", "cent"), 0, 0, tiled=True)
    proto, red = call(unpack, (back, key), [f32(1, docs)] * 2, "unpack", 1 << 20)
    return proto.reshape(docs), red.reshape(docs), stats


def local_general(documents, assigned, centroids, owner_slot):
    doc_count, width = documents.shape
    table_rows = centroids.shape[0]
    dp_count = lax.axis_size("dp")
    cent_count = lax.axis_size("cent")
    owner_count = dp_count * cent_count
    pair_cap = 2 * doc_count // owner_count
    row_cap = 5 * cent_count * pair_cap // 8
    slot_ids = owner_slot[assigned]
    owner_ids = slot_ids // table_rows
    local_ids = slot_ids % table_rows
    row_ids = owner_ids // cent_count
    col_ids = owner_ids % cent_count
    first_pos = bucket_positions(row_ids, dp_count, row_cap)
    outgoing = jnp.zeros((dp_count * row_cap, width), jnp.bfloat16).at[first_pos].set(documents)
    tag_ids = (
        jnp.full((dp_count * row_cap,), -1, jnp.int32)
        .at[first_pos]
        .set(col_ids * table_rows + local_ids)
    )
    relayed, relayed_tags = (
        lax.all_to_all(
            outgoing.reshape(dp_count, row_cap, width),
            "dp",
            split_axis=0,
            concat_axis=0,
            tiled=True,
        ),
        lax.all_to_all(
            tag_ids.reshape(dp_count, row_cap), "dp", split_axis=0, concat_axis=0, tiled=True
        ),
    )
    relayed = relayed.reshape(-1, width)
    relayed_tags = relayed_tags.reshape(-1)
    relay_live = relayed_tags >= 0
    relay_target = jnp.where(relay_live, relayed_tags // table_rows, cent_count)
    inner_cap = dp_count * pair_cap
    second_pos = bucket_positions(relay_target, cent_count, inner_cap)
    forward = (
        jnp.zeros((cent_count * inner_cap, width), jnp.bfloat16)
        .at[second_pos]
        .set(relayed, mode="drop")
    )
    forward_tags = (
        jnp.full((cent_count * inner_cap,), -1, jnp.int32)
        .at[second_pos]
        .set(jnp.where(relay_live, relayed_tags % table_rows, -1), mode="drop")
    )
    incoming, incoming_tags = (
        lax.all_to_all(
            forward.reshape(cent_count, inner_cap, width),
            "cent",
            split_axis=0,
            concat_axis=0,
            tiled=True,
        ),
        lax.all_to_all(
            forward_tags.reshape(cent_count, inner_cap),
            "cent",
            split_axis=0,
            concat_axis=0,
            tiled=True,
        ),
    )
    cluster_totals, proto_score, redundant = owner_work(
        incoming.reshape(-1, width), incoming_tags.reshape(-1), centroids
    )
    back_score, back_redundant = (
        lax.all_to_all(
            proto_score.reshape(cent_count, inner_cap),
            "cent",
            split_axis=0,
            concat_axis=0,
            tiled=True,
        ),
        lax.all_to_all(
            redundant.reshape(cent_count, inner_cap),
            "cent",
            split_axis=0,
            concat_axis=0,
            tiled=True,
        ),
    )
    safe_pos = jnp.clip(second_pos, 0, cent_count * inner_cap - 1)
    relay_score = jnp.where(relay_live, back_score.reshape(-1)[safe_pos], 0.0)
    relay_redundant = jnp.where(relay_live, back_redundant.reshape(-1)[safe_pos], 0.0)
    home_score, home_redundant = (
        lax.all_to_all(
            relay_score.reshape(dp_count, row_cap), "dp", split_axis=0, concat_axis=0, tiled=True
        ),
        lax.all_to_all(
            relay_redundant.reshape(dp_count, row_cap),
            "dp",
            split_axis=0,
            concat_axis=0,
            tiled=True,
        ),
    )
    prototypicality = home_score.reshape(-1)[first_pos]
    redundancy = home_redundant.reshape(-1)[first_pos]
    return (prototypicality, redundancy, cluster_totals)


def solution(mesh):
    in_specs = (P(("dp", "cent"), None), P(("dp", "cent")), P(("dp", "cent"), None), P())
    out_specs = (P(("dp", "cent")), P(("dp", "cent")), P(None, ("dp", "cent")))
    dp, cent = mesh.shape["dp"], mesh.shape["cent"]
    small = dp <= 8 and dp & (dp - 1) == 0 and cent & (cent - 1) == 0 and dp * cent > 1
    body = local if small else local_general
    return jax.shard_map(body, mesh=mesh, in_specs=in_specs, out_specs=out_specs, check_vma=False)
```

```python
import math

import jax
import jax.numpy as jnp
from jax import lax
from jax.experimental import pallas as pl
from jax.experimental.pallas import tpu as pltpu
from jax.sharding import PartitionSpec as P


LANES = 128
HIGHEST = lax.Precision.HIGHEST


def bucket_positions(target, groups, capacity):
    length = target.shape[0]
    indicator = (target[:, None] == jnp.arange(groups, dtype=jnp.int32)[None, :]).astype(
        jnp.bfloat16
    )
    earlier = (
        lax.broadcasted_iota(jnp.int32, (length, length), 0)
        > lax.broadcasted_iota(jnp.int32, (length, length), 1)
    ).astype(jnp.bfloat16)
    before = jnp.dot(earlier, indicator, preferred_element_type=jnp.float32)
    rank_ids = jnp.sum(before * indicator.astype(jnp.float32), axis=1).astype(jnp.int32)
    return jnp.where(target < groups, target * capacity + rank_ids, groups * capacity)


def owner_work(incoming, incoming_tags, centroids):
    table_rows = centroids.shape[0]
    width = incoming.shape[1]
    length = incoming_tags.shape[0]
    is_live = incoming_tags >= 0
    safe_slot = jnp.clip(incoming_tags, 0, table_rows - 1)
    cent_sq = jnp.einsum("kd,kd->k", centroids, centroids, preferred_element_type=jnp.float32)
    cent_vec = centroids[safe_slot]
    cross_dot = jnp.einsum("sd,sd->s", incoming, cent_vec, preferred_element_type=jnp.float32)
    self_sq = jnp.einsum("sd,sd->s", incoming, incoming, preferred_element_type=jnp.float32)
    inverse_norm = lax.rsqrt(self_sq + 1.0)
    similarity = cross_dot * inverse_norm * lax.rsqrt(cent_sq[safe_slot] + 1.0)
    members = (incoming_tags[:, None] == jnp.arange(table_rows, dtype=jnp.int32)[None, :]).astype(
        jnp.float32
    )
    live_weight = is_live.astype(jnp.float32)
    moments = jnp.stack(
        [live_weight, live_weight * similarity, live_weight * similarity * similarity]
    )
    cluster_totals = jnp.dot(
        moments, members, precision=lax.Precision.HIGHEST, preferred_element_type=jnp.float32
    )
    count_floor = jnp.maximum(cluster_totals[0], 1.0)
    mean_sim = cluster_totals[1] / count_floor
    variance = jnp.maximum(cluster_totals[2] / count_floor - mean_sim * mean_sim, 0.0)
    proto_score = jnp.where(
        is_live,
        (mean_sim[safe_slot] - similarity) / jnp.sqrt(variance[safe_slot] + 1.0 / width),
        0.0,
    )
    gram_block = lax.dot_general(
        incoming, incoming, (((1,), (1,)), ((), ())), preferred_element_type=jnp.float32
    )
    cosine = gram_block * inverse_norm[:, None] * inverse_norm[None, :]
    not_self = lax.broadcasted_iota(jnp.int32, (length, length), 0) != lax.broadcasted_iota(
        jnp.int32, (length, length), 1
    )
    same_cluster = (incoming_tags[:, None] == incoming_tags[None, :]) & is_live[:, None] & not_self
    redundant = math.sqrt(width) * jnp.max(jnp.where(same_cluster, cosine, 0.0), axis=1)
    return (cluster_totals, proto_score, redundant)


def iota(shape, dim):
    return lax.broadcasted_iota(jnp.int32, shape, dim)


def mm(a, b, dims, precision=None):
    return lax.dot_general(
        a, b, (dims, ((), ())), precision=precision, preferred_element_type=jnp.float32
    )


def ring(dp):
    line = dp >> 1
    return line ^ (line >> 1)


def shift(dp, m):
    place = (ring(dp) + (m >> 1)) & 3
    return ((place ^ (place >> 1)) << 1) | ((dp ^ m) & 1)


def back_shift(dp, m):
    return shift(dp, ((8 - (m & 6)) & 6) | (m & 1))


def relative(owner_dp, dp):
    return (((ring(owner_dp) - ring(dp)) & 3) << 1) | ((owner_dp ^ dp) & 1)


def params(mib):
    return pltpu.CompilerParams(vmem_limit_bytes=mib * 1024 * 1024)


def local(documents, assigned, centroids, owner_slot):
    docs, width = documents.shape
    rows = centroids.shape[0]
    dp = lax.axis_size("dp")
    cent = lax.axis_size("cent")
    owners = dp * cent
    cap = 2 * docs // owners
    row_cap = 5 * cent * cap // 8
    group = cent * cap
    clusters = owner_slot.shape[0]
    root = math.sqrt(width)
    far, direct, relayed, stages = plan()
    source = lambda m, e: back_shift(lax.axis_index("dp"), m) * cent + (lax.axis_index("cent") ^ e)
    span = lambda f: (f[1] * width // f[2], (f[1] + 1) * width // f[2])

    def route(assigned_hbm, table_hbm, docs_hbm, far_ref, tag_ref, key_ref, *scratch):
        assigned_ref, table_ref, docs_ref, sems = scratch
        copies = [
            pltpu.make_async_copy(src, dst, sems.at[n])
            for n, (src, dst) in enumerate(
                [(assigned_hbm, assigned_ref), (table_hbm, table_ref), (docs_hbm, docs_ref)]
            )
        ]
        for copy in copies:
            copy.start()
        copies[0].wait()
        copies[1].wait()
        a = assigned_ref[...]
        pick = (iota((clusters // LANES, docs), 0) == a // LANES).astype(jnp.float32)
        lines = mm(table_ref[...].astype(jnp.float32), pick, ((0,), (0,)), HIGHEST)
        slot = jnp.sum(
            jnp.where(iota((LANES, docs), 0) == a % LANES, lines, 0.0), axis=0, keepdims=True
        )
        owner = jnp.floor((slot + 0.5) * (1.0 / rows))
        home = slot - owner * rows + 1.0
        owner = owner.astype(jnp.int32)
        here, side = lax.axis_index("dp"), lax.axis_index("cent")
        rel = relative(owner // cent, here) * cent + ((owner % cent) ^ side)
        which = iota((owners, docs), 0)
        mine = which == owner
        near = which // cent == owner // cent
        earlier = (iota((docs, docs), 0) < iota((docs, docs), 1)).astype(jnp.bfloat16)
        before = mm(mine.astype(jnp.bfloat16), earlier, ((1,), (0,)))
        count = lambda m: jnp.sum(jnp.where(m, before, 0.0), axis=0, keepdims=True)
        rank = count(mine).astype(jnp.int32)
        row_rank = count(near).astype(jnp.int32)
        key = rel * cap + rank
        row_key = (rel // cent) * row_cap + row_rank
        key_ref[0:1, :] = key
        key_ref[1:2, :] = row_key
        key_ref[2:3, :] = owner
        at_rank = (iota((cap, docs), 0) == rank).astype(jnp.float32)
        at_row = (iota((row_cap, docs), 0) == row_rank).astype(jnp.float32)
        homes = mm(jnp.where(mine, home, 0.0), at_rank, ((1,), (1,)), HIGHEST)
        inner = (key % group + 1).astype(jnp.float32)
        inners = mm(jnp.where(near, inner, 0.0), at_row, ((1,), (1,)), HIGHEST)
        tag_ref[...] = jnp.zeros((owners, 1, LANES), jnp.int32)
        tag_ref[:, 0, :cap] = homes.astype(jnp.int32)
        tag_ref[:, 0, cap : cap + row_cap] = inners.astype(jnp.int32)
        sel = iota((row_cap, docs), 0) + far[0][0] * row_cap == row_key
        copies[2].wait()
        picked = mm(sel.astype(jnp.bfloat16), docs_ref[...], ((1,), (0,)))
        far_ref[...] = picked.astype(jnp.bfloat16)

    def pack(key_hbm, docs_hbm, *refs):
        *outs, key_ref, docs_ref, sems = refs
        copies = [
            pltpu.make_async_copy(key_hbm, key_ref, sems.at[0]),
            pltpu.make_async_copy(docs_hbm, docs_ref, sems.at[1]),
        ]
        for copy in copies:
            copy.start()
        copies[0].wait()
        key, row_key = key_ref[0:1, :], key_ref[1:2, :]
        rest = sorted({f[0] for f in far[1:]})
        sel = [iota((row_cap, docs), 0) + m * row_cap == row_key for m in rest]
        sel += [iota((group, docs), 0) + m * group == key for m in direct]
        sel = jnp.concatenate([v.astype(jnp.bfloat16) for v in sel], axis=0)
        copies[1].wait()
        step = width // 4
        for lo in range(0, width, step):
            picked = mm(sel, docs_ref[:, lo : lo + step], ((1,), (0,))).astype(jnp.bfloat16)
            for ref, f in zip(outs, far[1:]):
                at = rest.index(f[0]) * row_cap
                if span(f)[0] <= lo < span(f)[1]:
                    lane = lo - span(f)[0]
                    ref[:, lane : lane + step] = picked[at : at + row_cap]
            for n, ref in enumerate(outs[len(far) - 1 :]):
                at = len(rest) * row_cap + n * cap
                ref[:, lo : lo + step] = picked[at : at + cap]

    def norms(cent_ref, keep_ref, inv_ref):
        keep_ref[...] = cent_ref[...]
        c = cent_ref[...].astype(jnp.float32)
        inv_ref[...] = lax.rsqrt(jnp.sum(c * c, axis=1, keepdims=True) + 1.0)

    def make_relay(part):
        def body(tag_ref, *refs):
            for n, (m, _, _) in enumerate(part):
                tags = tag_ref[pl.ds(source(m, 0), 1), 0, cap : cap + row_cap]
                sel = (iota((group, row_cap), 0) + 1 == tags).astype(jnp.bfloat16)
                picked = mm(sel, refs[n][...], ((1,), (0,))).astype(jnp.bfloat16)
                for e in range(cent):
                    refs[len(part) + e][n * cap : (n + 1) * cap] = picked[e * cap : (e + 1) * cap]

        return body

    def make_owner(s):
        parts = stages[s]
        masks = stage_masks(parts)
        fresh = len(masks) * group
        last = s == len(stages) - 1

        def body(*refs):
            refs = list(refs)
            take = lambda n: [refs.pop(0) for _ in range(n)]
            arrays = [take(cent) for _ in parts]
            tag_ref, cent_ref, cent_inv_ref = take(3)
            olds = [take(3) for _ in range(s)]
            tally = take(1)[0] if s else None
            if last:
                score_ref, stat_ref, x = take(3)
            else:
                x, col, line, tally_out = take(4)
                old_outs = take(s)
            for part, refs_e in zip(parts, arrays):
                for i, f in enumerate(part):
                    lo, hi = span(f)
                    for e in range(cent):
                        at = (masks.index(f[0]) * cent + e) * cap
                        x[at : at + cap, lo:hi] = refs_e[e][i * cap : (i + 1) * cap, :]
            tags = [
                tag_ref[pl.ds(source(m, e), 1), 0, :cap] for m in masks for e in range(cent)
            ]
            tag = jnp.concatenate(tags, axis=1).astype(jnp.float32)
            eye = iota((LANES, LANES), 0) == iota((LANES, LANES), 1)

            def to_row(v):
                pieces = [
                    jnp.sum(jnp.where(eye, v[i : i + LANES], 0.0), axis=0, keepdims=True)
                    for i in range(0, v.shape[0], LANES)
                ]
                return jnp.concatenate(pieces, axis=1) if len(pieces) > 1 else pieces[0]

            def to_col(v):
                pieces = [
                    jnp.sum(jnp.where(eye, v[:, i : i + LANES], 0.0), axis=1, keepdims=True)
                    for i in range(0, v.shape[1], LANES)
                ]
                return jnp.concatenate(pieces, axis=0) if len(pieces) > 1 else pieces[0]

            cent_inv = cent_inv_ref[...]
            if s == 0:
                counts = [jnp.zeros((rows, 1), jnp.float32)] * 3
            else:
                counts = [tally[:, i : i + 1] for i in range(3)]
            xn = x[...]
            own_gram = mm(xn, xn, ((1,), (1,)))
            cols, lines = [], []
            for i in range(0, fresh, LANES):
                diag = jnp.where(eye, own_gram[i : i + LANES, i : i + LANES], 0.0)
                cols.append(lax.rsqrt(jnp.sum(diag, axis=1, keepdims=True) + 1.0))
                lines.append(lax.rsqrt(jnp.sum(diag, axis=0, keepdims=True) + 1.0))
            tag_col = to_col(tag)
            inv_col = jnp.concatenate(cols, axis=0)
            inv = jnp.concatenate(lines, axis=1)
            cross = mm(cent_ref[...], xn, ((1,), (1,)))
            own = (iota((rows, fresh), 0) + 1).astype(jnp.float32) == tag
            sim = jnp.sum(jnp.where(own, cross * cent_inv, 0.0), axis=0, keepdims=True) * inv
            add = lambda v: jnp.sum(jnp.where(own, v, 0.0), axis=1, keepdims=True)
            counts = [c + add(v) for c, v in zip(counts, (jnp.ones_like(sim), sim, sim * sim))]
            same = (tag_col == tag) & (iota((fresh, fresh), 0) != iota((fresh, fresh), 1))
            best = jnp.max(jnp.where(same, own_gram * inv_col, 0.0), axis=0, keepdims=True)
            old_best = []
            for x_old, col_old, line_old in olds:
                gram = mm(x_old[...], xn, ((1,), (1,)))
                same = col_old[:, 0:1] == tag
                up = jnp.max(
                    jnp.where(same, gram * col_old[:, 1:2], 0.0), axis=0, keepdims=True
                )
                best = jnp.maximum(best, up)
                down = jnp.max(jnp.where(same, gram * inv, 0.0), axis=1, keepdims=True)
                old_best.append(jnp.maximum(line_old[3:4, :], to_row(down)))
            if not last:
                col[:, 0:1] = tag_col
                col[:, 1:2] = inv_col
                for i, v in enumerate((tag, inv, sim, best)):
                    line[i : i + 1, :] = v
                for i, v in enumerate(counts):
                    tally_out[:, i : i + 1] = v
                for ref, (_, _, line_old), v in zip(old_outs, olds, old_best):
                    ref[0:3, :] = line_old[0:3, :]
                    ref[3:4, :] = v
                return
            floor = jnp.maximum(counts[0], 1.0)
            mean = counts[1] / floor
            var = jnp.maximum(counts[2] / floor - mean * mean, 0.0)
            spread = 1.0 / jnp.sqrt(var + 1.0 / width)
            for i, v in enumerate(counts):
                stat_ref[i : i + 1, :] = to_row(v)
            facts = [(l[0:1, :], l[1:2, :], l[2:3, :], b) for (_, _, l), b in zip(olds, old_best)]
            facts.append((tag, inv, sim, best))
            for parts_s, (tag, inv, sim, best) in zip(stages, facts):
                order_s = stage_masks(parts_s)
                own = (iota((rows, tag.shape[1]), 0) + 1).astype(jnp.float32) == tag
                pick = lambda v: jnp.sum(jnp.where(own, v, 0.0), axis=0, keepdims=True)
                score = (pick(mean) - sim) * pick(spread)
                red = best * inv * root
                for b in range(len(order_s) * cent):
                    part = slice(b * cap, (b + 1) * cap)
                    score_ref[pl.ds(source(order_s[b // cent], b % cent), 1), 0, :] = jnp.concatenate(
                        [score[:, part], red[:, part]], axis=1
                    )

        return body

    def unpack(score_ref, key_ref, out_ref, red_ref):
        key = key_ref[0:1, :]
        pick = (iota((owners, docs), 0) == key_ref[2:3, :]).astype(jnp.float32)
        got = mm(score_ref[:, 0, :], pick, ((0,), (0,)), HIGHEST)
        rank = iota((2 * cap, docs), 0)
        out_ref[...] = jnp.sum(jnp.where(rank == key % cap, got, 0.0), axis=0, keepdims=True)
        red_ref[...] = jnp.sum(jnp.where(rank == key % cap + cap, got, 0.0), axis=0, keepdims=True)

    f32 = lambda *s: jax.ShapeDtypeStruct(s, jnp.float32)
    bf16 = lambda *s: jax.ShapeDtypeStruct(s, jnp.bfloat16)
    i32 = lambda *s: jax.ShapeDtypeStruct(s, jnp.int32)
    cost = lambda n: pl.CostEstimate(flops=n, bytes_accessed=1 << 20, transcendentals=0)

    def call(body, ins, outs, flops, scratch=(), mib=16, space=pltpu.VMEM):
        return pl.pallas_call(
            body,
            out_shape=outs,
            in_specs=[pl.BlockSpec(memory_space=space)] * len(ins),
            out_specs=[pl.BlockSpec(memory_space=pltpu.VMEM)] * len(outs),
            scratch_shapes=list(scratch),
            compiler_params=params(mib),
            cost_estimate=cost(flops),
        )(*ins)

    def send(value, m, e):
        if not m and not e:
            return value
        if not e:
            return lax.ppermute(value, "dp", [(i, shift(i, m)) for i in range(dp)])
        if not m:
            return lax.ppermute(value, "cent", [(j, j ^ e) for j in range(cent)])
        pairs = [
            (i * cent + j, shift(i, m) * cent + (j ^ e)) for i in range(dp) for j in range(cent)
        ]
        return lax.ppermute(value, ("dp", "cent"), pairs)

    def exchange(value):
        return lax.all_to_all(value, ("dp", "cent"), 0, 0, tiled=True)

    table = owner_slot.reshape(-1, LANES)
    held = pltpu.VMEM((docs, width), jnp.bfloat16)
    first, tags, key = call(
        route,
        (assigned.reshape(1, docs), table, documents),
        [bf16(row_cap, width), i32(owners, 1, LANES), i32(8, docs)],
        2 * row_cap * docs * width,
        [
            pltpu.VMEM((1, docs), jnp.int32),
            pltpu.VMEM(table.shape, jnp.int32),
            held,
            pltpu.SemaphoreType.DMA((3,)),
        ],
        mib=63,
        space=pl.ANY,
    )
    tags = exchange(tags)
    got = call(
        pack,
        (key, documents),
        [bf16(row_cap, width // f[2]) for f in far[1:]]
        + [bf16(cap, width)] * (len(direct) * cent),
        2 * len(far) * row_cap * docs * width,
        [pltpu.VMEM((8, docs), jnp.int32), held, pltpu.SemaphoreType.DMA((2,))],
        mib=63,
        space=pl.ANY,
    )
    sent = {f: send(v, f[0], 0) for f, v in zip(far, [first, *got])}
    arrays = {}
    for n, m in enumerate(direct):
        near = got[len(far) - 1 + n * cent : len(far) - 1 + (n + 1) * cent]
        arrays[((m, 0, 1),)] = [send(v, m, e) for e, v in enumerate(near)]
    for part in relayed:
        size = width // part[0][2]
        hop = call(
            make_relay(part),
            (tags, *[sent[f] for f in part]),
            [bf16(len(part) * cap, size)] * cent,
            2 * len(part) * group * row_cap * size,
        )
        arrays[part] = [send(hop[e], 0, e) for e in range(cent)]
    kept, cent_inv = call(norms, (centroids,), [bf16(rows, width), f32(rows, 1)], 2 * rows * width)
    olds, tally = [], None
    for s, parts in enumerate(stages):
        fresh = len(stage_masks(parts)) * group
        ins = [b for part in parts for b in arrays[part]] + [tags, kept, cent_inv]
        ins += [v for old in olds for v in old] + ([tally] if s else [])
        flops = 2 * fresh * (rows + fresh + sum(o[0].shape[0] for o in olds)) * width
        if s < len(stages) - 1:
            outs = [bf16(fresh, width), f32(fresh, 2), f32(4, fresh), f32(rows, 3)]
            outs += [f32(*o[2].shape) for o in olds]
            x, col, line, tally, *lines = call(make_owner(s), ins, outs, flops)
            olds = [(o[0], o[1], l) for o, l in zip(olds, lines)] + [(x, col, line)]
        else:
            scratch = [pltpu.VMEM((fresh, width), jnp.bfloat16)]
            outs = [f32(owners, 1, 2 * cap), f32(3, rows)]
            scores, stats = call(make_owner(s), ins, outs, flops, scratch)
    back = exchange(scores)
    proto, red = call(unpack, (back, key), [f32(1, docs)] * 2, 1 << 20)
    return proto.reshape(docs), red.reshape(docs), stats


def stage_masks(parts):
    out = []
    for part in parts:
        out += [f[0] for f in part if f[0] not in out]
    return out


def plan():
    whole = lambda *masks: tuple((m, 0, 1) for m in masks)
    lo, hi = (5, 0, 2), (5, 1, 2)
    far = [f[0] for f in map(whole, (4, 2, 6, 3, 7))] + [lo, hi]
    relayed = [(f,) for f in far]
    direct = [0, 1]
    stages = [
        [whole(0), whole(1)],
        [whole(4), whole(2), whole(6)],
        [whole(3), whole(7)],
        [(lo,), (hi,)],
    ]
    return far, direct, relayed, stages


def local_general(documents, assigned, centroids, owner_slot):
    doc_count, width = documents.shape
    table_rows = centroids.shape[0]
    dp_count = lax.axis_size("dp")
    cent_count = lax.axis_size("cent")
    owner_count = dp_count * cent_count
    pair_cap = 2 * doc_count // owner_count
    row_cap = 5 * cent_count * pair_cap // 8
    slot_ids = owner_slot[assigned]
    owner_ids = slot_ids // table_rows
    local_ids = slot_ids % table_rows
    row_ids = owner_ids // cent_count
    col_ids = owner_ids % cent_count
    first_pos = bucket_positions(row_ids, dp_count, row_cap)
    outgoing = jnp.zeros((dp_count * row_cap, width), jnp.bfloat16).at[first_pos].set(documents)
    tag_ids = (
        jnp.full((dp_count * row_cap,), -1, jnp.int32)
        .at[first_pos]
        .set(col_ids * table_rows + local_ids)
    )
    relayed, relayed_tags = (
        lax.all_to_all(
            outgoing.reshape(dp_count, row_cap, width),
            "dp",
            split_axis=0,
            concat_axis=0,
            tiled=True,
        ),
        lax.all_to_all(
            tag_ids.reshape(dp_count, row_cap), "dp", split_axis=0, concat_axis=0, tiled=True
        ),
    )
    relayed = relayed.reshape(-1, width)
    relayed_tags = relayed_tags.reshape(-1)
    relay_live = relayed_tags >= 0
    relay_target = jnp.where(relay_live, relayed_tags // table_rows, cent_count)
    inner_cap = dp_count * pair_cap
    second_pos = bucket_positions(relay_target, cent_count, inner_cap)
    forward = (
        jnp.zeros((cent_count * inner_cap, width), jnp.bfloat16)
        .at[second_pos]
        .set(relayed, mode="drop")
    )
    forward_tags = (
        jnp.full((cent_count * inner_cap,), -1, jnp.int32)
        .at[second_pos]
        .set(jnp.where(relay_live, relayed_tags % table_rows, -1), mode="drop")
    )
    incoming, incoming_tags = (
        lax.all_to_all(
            forward.reshape(cent_count, inner_cap, width),
            "cent",
            split_axis=0,
            concat_axis=0,
            tiled=True,
        ),
        lax.all_to_all(
            forward_tags.reshape(cent_count, inner_cap),
            "cent",
            split_axis=0,
            concat_axis=0,
            tiled=True,
        ),
    )
    cluster_totals, proto_score, redundant = owner_work(
        incoming.reshape(-1, width), incoming_tags.reshape(-1), centroids
    )
    back_score, back_redundant = (
        lax.all_to_all(
            proto_score.reshape(cent_count, inner_cap),
            "cent",
            split_axis=0,
            concat_axis=0,
            tiled=True,
        ),
        lax.all_to_all(
            redundant.reshape(cent_count, inner_cap),
            "cent",
            split_axis=0,
            concat_axis=0,
            tiled=True,
        ),
    )
    safe_pos = jnp.clip(second_pos, 0, cent_count * inner_cap - 1)
    relay_score = jnp.where(relay_live, back_score.reshape(-1)[safe_pos], 0.0)
    relay_redundant = jnp.where(relay_live, back_redundant.reshape(-1)[safe_pos], 0.0)
    home_score, home_redundant = (
        lax.all_to_all(
            relay_score.reshape(dp_count, row_cap), "dp", split_axis=0, concat_axis=0, tiled=True
        ),
        lax.all_to_all(
            relay_redundant.reshape(dp_count, row_cap),
            "dp",
            split_axis=0,
            concat_axis=0,
            tiled=True,
        ),
    )
    prototypicality = home_score.reshape(-1)[first_pos]
    redundancy = home_redundant.reshape(-1)[first_pos]
    return (prototypicality, redundancy, cluster_totals)


def solution(mesh):
    in_specs = (P(("dp", "cent"), None), P(("dp", "cent")), P(("dp", "cent"), None), P())
    out_specs = (P(("dp", "cent")), P(("dp", "cent")), P(None, ("dp", "cent")))
    dp, cent = mesh.shape["dp"], mesh.shape["cent"]
    small = dp == 8 and cent & (cent - 1) == 0

    def body(*args):
        return (local if small else local_general)(*args)

    return jax.shard_map(body, mesh=mesh, in_specs=in_specs, out_specs=out_specs, check_vma=False)
```

```python
import math

import jax
import jax.numpy as jnp
from jax import lax
from jax.experimental import pallas as pl
from jax.experimental.pallas import tpu as pltpu
from jax.sharding import PartitionSpec as P


LANES = 128
HIGHEST = lax.Precision.HIGHEST


def bucket_positions(target, groups, capacity):
    length = target.shape[0]
    indicator = (target[:, None] == jnp.arange(groups, dtype=jnp.int32)[None, :]).astype(
        jnp.bfloat16
    )
    earlier = (
        lax.broadcasted_iota(jnp.int32, (length, length), 0)
        > lax.broadcasted_iota(jnp.int32, (length, length), 1)
    ).astype(jnp.bfloat16)
    before = jnp.dot(earlier, indicator, preferred_element_type=jnp.float32)
    rank_ids = jnp.sum(before * indicator.astype(jnp.float32), axis=1).astype(jnp.int32)
    return jnp.where(target < groups, target * capacity + rank_ids, groups * capacity)


def owner_work(incoming, incoming_tags, centroids):
    table_rows = centroids.shape[0]
    width = incoming.shape[1]
    length = incoming_tags.shape[0]
    is_live = incoming_tags >= 0
    safe_slot = jnp.clip(incoming_tags, 0, table_rows - 1)
    cent_sq = jnp.einsum("kd,kd->k", centroids, centroids, preferred_element_type=jnp.float32)
    cent_vec = centroids[safe_slot]
    cross_dot = jnp.einsum("sd,sd->s", incoming, cent_vec, preferred_element_type=jnp.float32)
    self_sq = jnp.einsum("sd,sd->s", incoming, incoming, preferred_element_type=jnp.float32)
    inverse_norm = lax.rsqrt(self_sq + 1.0)
    similarity = cross_dot * inverse_norm * lax.rsqrt(cent_sq[safe_slot] + 1.0)
    members = (incoming_tags[:, None] == jnp.arange(table_rows, dtype=jnp.int32)[None, :]).astype(
        jnp.float32
    )
    live_weight = is_live.astype(jnp.float32)
    moments = jnp.stack(
        [live_weight, live_weight * similarity, live_weight * similarity * similarity]
    )
    cluster_totals = jnp.dot(
        moments, members, precision=lax.Precision.HIGHEST, preferred_element_type=jnp.float32
    )
    count_floor = jnp.maximum(cluster_totals[0], 1.0)
    mean_sim = cluster_totals[1] / count_floor
    variance = jnp.maximum(cluster_totals[2] / count_floor - mean_sim * mean_sim, 0.0)
    proto_score = jnp.where(
        is_live,
        (mean_sim[safe_slot] - similarity) / jnp.sqrt(variance[safe_slot] + 1.0 / width),
        0.0,
    )
    gram_block = lax.dot_general(
        incoming, incoming, (((1,), (1,)), ((), ())), preferred_element_type=jnp.float32
    )
    cosine = gram_block * inverse_norm[:, None] * inverse_norm[None, :]
    not_self = lax.broadcasted_iota(jnp.int32, (length, length), 0) != lax.broadcasted_iota(
        jnp.int32, (length, length), 1
    )
    same_cluster = (incoming_tags[:, None] == incoming_tags[None, :]) & is_live[:, None] & not_self
    redundant = math.sqrt(width) * jnp.max(jnp.where(same_cluster, cosine, 0.0), axis=1)
    return (cluster_totals, proto_score, redundant)


def iota(shape, dim):
    return lax.broadcasted_iota(jnp.int32, shape, dim)


def mm(a, b, dims, precision=None):
    return lax.dot_general(
        a, b, (dims, ((), ())), precision=precision, preferred_element_type=jnp.float32
    )


def ring(dp):
    line = dp >> 1
    return line ^ (line >> 1)


def shift(dp, m):
    place = (ring(dp) + (m >> 1)) & 3
    return ((place ^ (place >> 1)) << 1) | ((dp ^ m) & 1)


def back_shift(dp, m):
    return shift(dp, ((8 - (m & 6)) & 6) | (m & 1))


def relative(owner_dp, dp):
    return (((ring(owner_dp) - ring(dp)) & 3) << 1) | ((owner_dp ^ dp) & 1)


def params(mib):
    return pltpu.CompilerParams(vmem_limit_bytes=mib * 1024 * 1024)


def local(documents, assigned, centroids, owner_slot):
    docs, width = documents.shape
    rows = centroids.shape[0]
    dp = lax.axis_size("dp")
    cent = lax.axis_size("cent")
    owners = dp * cent
    cap = 2 * docs // owners
    row_cap = 5 * cent * cap // 8
    group = cent * cap
    clusters = owner_slot.shape[0]
    root = math.sqrt(width)
    far, direct, relayed, stages = plan()
    source = lambda m, e: back_shift(lax.axis_index("dp"), m) * cent + (lax.axis_index("cent") ^ e)
    span = lambda f: (f[1] * width // 4, f[2] * width // 4)
    size = lambda f: span(f)[1] - span(f)[0]

    def route(assigned_hbm, table_hbm, docs_hbm, far_ref, tag_ref, key_ref, *scratch):
        assigned_ref, table_ref, docs_ref, sems = scratch
        copies = [
            pltpu.make_async_copy(src, dst, sems.at[n])
            for n, (src, dst) in enumerate(
                [(assigned_hbm, assigned_ref), (table_hbm, table_ref), (docs_hbm, docs_ref)]
            )
        ]
        for copy in copies:
            copy.start()
        copies[0].wait()
        copies[1].wait()
        a = assigned_ref[...]
        pick = (iota((clusters // LANES, docs), 0) == a // LANES).astype(jnp.bfloat16)
        digits, left = [], clusters - 1
        while left:
            digits.append((table_ref[...] >> (7 * len(digits))) & (LANES - 1))
            left >>= 7
        digits = [d.astype(jnp.float32).astype(jnp.bfloat16) for d in digits]
        lines = mm(jnp.concatenate(digits, axis=1), pick, ((0,), (0,)))
        value = lines[:LANES]
        for n in range(1, len(digits)):
            value = value + lines[n * LANES : (n + 1) * LANES] * float(LANES**n)
        slot = jnp.sum(
            jnp.where(iota((LANES, docs), 0) == a % LANES, value, 0.0), axis=0, keepdims=True
        )
        owner = jnp.floor((slot + 0.5) * (1.0 / rows))
        home = (slot - owner * rows).astype(jnp.int32) + 1
        owner = owner.astype(jnp.int32)
        here, side = lax.axis_index("dp"), lax.axis_index("cent")
        rel = relative(owner // cent, here) * cent + ((owner % cent) ^ side)
        which = iota((owners, docs), 0)
        mine = which == owner
        near = which // cent == owner // cent
        earlier = (iota((LANES, LANES), 0) < iota((LANES, LANES), 1)).astype(jnp.bfloat16)
        marks = mine.astype(jnp.float32)
        before, total = [], jnp.zeros((owners, 1), jnp.float32)
        for lo in range(0, docs, LANES):
            part = marks[:, lo : lo + LANES]
            before.append(mm(part.astype(jnp.bfloat16), earlier, ((1,), (0,))) + total)
            total = total + jnp.sum(part, axis=1, keepdims=True)
        before = jnp.concatenate(before, axis=1)
        count = lambda m: jnp.sum(jnp.where(m, before, 0.0), axis=0, keepdims=True)
        rank = count(mine).astype(jnp.int32)
        row_rank = count(near).astype(jnp.int32)
        key = rel * cap + rank
        row_key = (rel // cent) * row_cap + row_rank
        key_ref[0:1, :] = key
        key_ref[1:2, :] = row_key
        key_ref[2:3, :] = owner
        spread = lambda m, v: jnp.where(m, v.astype(jnp.float32), 0.0).astype(jnp.bfloat16)
        at_rank = (iota((cap, docs), 0) == rank).astype(jnp.bfloat16)
        at_row = (iota((row_cap, docs), 0) == row_rank).astype(jnp.bfloat16)
        homes = jnp.concatenate([spread(mine, home // LANES), spread(mine, home % LANES)], axis=0)
        homes = mm(homes, at_rank, ((1,), (1,)))
        homes = homes[:owners] * float(LANES) + homes[owners:]
        inners = mm(spread(near, key % group + 1), at_row, ((1,), (1,)))
        tag_ref[...] = jnp.zeros((owners, 1, LANES), jnp.int32)
        tag_ref[:, 0, :cap] = homes.astype(jnp.int32)
        tag_ref[:, 0, cap : cap + row_cap] = inners.astype(jnp.int32)
        sel = iota((row_cap, docs), 0) + far[0][0] * row_cap == row_key
        copies[2].wait()
        picked = mm(sel.astype(jnp.bfloat16), docs_ref[...], ((1,), (0,)))
        far_ref[...] = picked.astype(jnp.bfloat16)

    def pack(key_hbm, docs_hbm, *refs):
        *outs, key_ref, docs_ref, sems = refs
        copies = [
            pltpu.make_async_copy(key_hbm, key_ref, sems.at[0]),
            pltpu.make_async_copy(docs_hbm, docs_ref, sems.at[1]),
        ]
        for copy in copies:
            copy.start()
        copies[0].wait()
        key, row_key = key_ref[0:1, :], key_ref[1:2, :]
        rest = sorted({f[0] for f in far[1:]})
        sel = [iota((row_cap, docs), 0) + m * row_cap == row_key for m in rest]
        sel += [iota((group, docs), 0) + m * group == key for m in direct]
        sel = jnp.concatenate([v.astype(jnp.bfloat16) for v in sel], axis=0)
        copies[1].wait()
        step = width // 4
        for lo in range(0, width, step):
            picked = mm(sel, docs_ref[:, lo : lo + step], ((1,), (0,))).astype(jnp.bfloat16)
            for ref, f in zip(outs, far[1:]):
                at = rest.index(f[0]) * row_cap
                if span(f)[0] <= lo < span(f)[1]:
                    lane = lo - span(f)[0]
                    ref[:, lane : lane + step] = picked[at : at + row_cap]
            for n, ref in enumerate(outs[len(far) - 1 :]):
                at = len(rest) * row_cap + n * cap
                ref[:, lo : lo + step] = picked[at : at + cap]

    def norms(cent_ref, keep_ref, inv_ref):
        keep_ref[...] = cent_ref[...]
        c = cent_ref[...].astype(jnp.float32)
        inv_ref[...] = lax.rsqrt(jnp.sum(c * c, axis=1, keepdims=True) + 1.0)

    def make_relay(part):
        def body(tag_ref, *refs):
            for n, (m, _, _) in enumerate(part):
                tags = tag_ref[pl.ds(source(m, 0), 1), 0, cap : cap + row_cap]
                sel = (iota((group, row_cap), 0) + 1 == tags).astype(jnp.bfloat16)
                picked = mm(sel, refs[n][...], ((1,), (0,))).astype(jnp.bfloat16)
                for e in range(cent):
                    refs[len(part) + e][n * cap : (n + 1) * cap] = picked[e * cap : (e + 1) * cap]

        return body

    def fill(x, parts, masks, arrays):
        start = span(parts[0][0])[0] if len(masks) == 1 else 0
        for part, refs in zip(parts, arrays):
            for i, f in enumerate(part):
                lo, hi = span(f)
                for e in range(cent):
                    at = (masks.index(f[0]) * cent + e) * cap
                    x[at : at + cap, lo - start : hi - start] = refs[e][i * cap : (i + 1) * cap, :]

    def partial(*refs):
        parts = stages[-1][:-1]
        refs = list(refs)
        arrays = [[refs.pop(0) for _ in range(cent)] for _ in parts]
        *lefts, acc_ref, x = refs
        fill(x, parts, stage_masks(parts), arrays)
        xn, base = x[...], 0
        for left in lefts:
            out = mm(left[:, : xn.shape[1]], xn, ((1,), (1,)))
            acc_ref[base : base + out.shape[0], :] = out
            base += out.shape[0]
        acc_ref[base:, :] = mm(xn, xn, ((1,), (1,)))

    def make_owner(s):
        parts = stages[s]
        masks = stage_masks(parts)
        fresh = len(masks) * group
        last = s == len(stages) - 1

        def body(*refs):
            refs = list(refs)
            take = lambda n: [refs.pop(0) for _ in range(n)]
            arrays = [take(cent) for _ in (parts[-1:] if last else parts)]
            tag_ref, cent_ref, cent_inv_ref = take(3)
            olds = [take(4) for _ in range(s)]
            tally = take(1)[0] if s else None
            acc_ref = take(1)[0] if last else None
            if last:
                score_ref, stat_ref, x = take(3)
            else:
                x, col, line, own_ref, tally_out = take(5)
                old_outs = take(s)
            fill(x, parts[-1:] if last else parts, masks, arrays)
            lane = slice(*span(parts[-1][0])) if last else slice(None)
            base = [0]

            def dots(left, right):
                out = mm(left[:, lane], right, ((1,), (1,)))
                if last:
                    out = out + acc_ref[base[0] : base[0] + out.shape[0], :]
                base[0] += out.shape[0]
                return out

            tags = [
                tag_ref[pl.ds(source(m, e), 1), 0, :cap] for m in masks for e in range(cent)
            ]
            tag = jnp.concatenate(tags, axis=1).astype(jnp.float32)
            eye = iota((LANES, LANES), 0) == iota((LANES, LANES), 1)

            def to_row(v):
                pieces = [
                    jnp.sum(jnp.where(eye, v[i : i + LANES], 0.0), axis=0, keepdims=True)
                    for i in range(0, v.shape[0], LANES)
                ]
                return jnp.concatenate(pieces, axis=1) if len(pieces) > 1 else pieces[0]

            def to_col(v):
                pieces = [
                    jnp.sum(jnp.where(eye, v[:, i : i + LANES], 0.0), axis=1, keepdims=True)
                    for i in range(0, v.shape[1], LANES)
                ]
                return jnp.concatenate(pieces, axis=0) if len(pieces) > 1 else pieces[0]

            cent_inv = cent_inv_ref[...]
            if s == 0:
                counts = [jnp.zeros((rows, 1), jnp.float32)] * 3
            else:
                counts = [tally[:, i : i + 1] for i in range(3)]
            xn = x[...]
            cross = dots(cent_ref, xn)
            grams = [dots(old[0], xn) for old in olds]
            own_gram = mm(xn, xn, ((1,), (1,))) + (acc_ref[base[0] :, :] if last else 0.0)
            cols, lines = [], []
            for i in range(0, fresh, LANES):
                diag = jnp.where(eye, own_gram[i : i + LANES, i : i + LANES], 0.0)
                cols.append(lax.rsqrt(jnp.sum(diag, axis=1, keepdims=True) + 1.0))
                lines.append(lax.rsqrt(jnp.sum(diag, axis=0, keepdims=True) + 1.0))
            tag_col = to_col(tag)
            inv_col = jnp.concatenate(cols, axis=0)
            inv = jnp.concatenate(lines, axis=1)
            own = (iota((rows, fresh), 0) + 1).astype(jnp.float32) == tag
            sim = jnp.sum(jnp.where(own, cross * cent_inv, 0.0), axis=0, keepdims=True) * inv
            add = lambda v: jnp.sum(jnp.where(own, v, 0.0), axis=1, keepdims=True)
            counts = [c + add(v) for c, v in zip(counts, (jnp.ones_like(sim), sim, sim * sim))]
            same = (tag_col == tag) & (iota((fresh, fresh), 0) != iota((fresh, fresh), 1))
            best = jnp.max(jnp.where(same, own_gram * inv_col, 0.0), axis=0, keepdims=True)
            old_best = []
            for gram, (_, col_old, line_old, _) in zip(grams, olds):
                same = col_old[:, 0:1] == tag
                up = jnp.max(
                    jnp.where(same, gram * col_old[:, 1:2], 0.0), axis=0, keepdims=True
                )
                best = jnp.maximum(best, up)
                down = jnp.max(jnp.where(same, gram * inv, 0.0), axis=1, keepdims=True)
                old_best.append(jnp.maximum(line_old[3:4, :], to_row(down)))
            if not last:
                col[:, 0:1] = tag_col
                col[:, 1:2] = inv_col
                for i, v in enumerate((tag, inv, sim, best)):
                    line[i : i + 1, :] = v
                for i, v in enumerate(counts):
                    tally_out[:, i : i + 1] = v
                own_ref[...] = own.astype(jnp.bfloat16)
                for ref, (_, _, line_old, _), v in zip(old_outs, olds, old_best):
                    ref[0:3, :] = line_old[0:3, :]
                    ref[3:4, :] = v
                return
            count, s1, s2 = [to_row(v) for v in counts]
            for i, v in enumerate((count, s1, s2)):
                stat_ref[i : i + 1, :] = v
            floor = jnp.maximum(count, 1.0)
            mean = s1 / floor
            var = jnp.maximum(s2 / floor - mean * mean, 0.0)
            terms = []
            for v in (mean, 1.0 / jnp.sqrt(var + 1.0 / width)):
                for _ in range(3):
                    terms.append(v.astype(jnp.bfloat16).astype(jnp.float32))
                    v = v - terms[-1]
            table = jnp.zeros((8, rows), jnp.float32)
            for i, v in enumerate(terms):
                table = jnp.where(iota((8, rows), 0) == i, v, table)
            table = table.astype(jnp.bfloat16)
            facts = [(l[1:2, :], l[2:3, :], v, o) for (_, _, l, o), v in zip(olds, old_best)]
            facts.append((inv, sim, best, own.astype(jnp.bfloat16)))
            for parts_s, (inv, sim, best, own) in zip(stages, facts):
                order_s = stage_masks(parts_s)
                got = mm(table, own[...], ((1,), (0,)))
                mean_d = got[0:1, :] + got[1:2, :] + got[2:3, :]
                spread_d = got[3:4, :] + got[4:5, :] + got[5:6, :]
                score = (mean_d - sim) * spread_d
                red = best * inv * root
                for b in range(len(order_s) * cent):
                    part = slice(b * cap, (b + 1) * cap)
                    score_ref[pl.ds(source(order_s[b // cent], b % cent), 1), 0, :] = jnp.concatenate(
                        [score[:, part], red[:, part]], axis=1
                    )

        return body

    def unpack(score_ref, key_ref, stat_ref, out_ref, red_ref, stat_out):
        stat_out[...] = stat_ref[...]
        key = key_ref[0:1, :]
        pick = (iota((owners, docs), 0) == key_ref[2:3, :]).astype(jnp.float32)
        got = mm(score_ref[:, 0, :], pick, ((0,), (0,)), HIGHEST)
        rank = iota((2 * cap, docs), 0)
        out_ref[...] = jnp.sum(jnp.where(rank == key % cap, got, 0.0), axis=0, keepdims=True)
        red_ref[...] = jnp.sum(jnp.where(rank == key % cap + cap, got, 0.0), axis=0, keepdims=True)

    f32 = lambda *s: jax.ShapeDtypeStruct(s, jnp.float32)
    bf16 = lambda *s: jax.ShapeDtypeStruct(s, jnp.bfloat16)
    i32 = lambda *s: jax.ShapeDtypeStruct(s, jnp.int32)
    cost = lambda n: pl.CostEstimate(flops=n, bytes_accessed=1 << 20, transcendentals=0)

    def call(body, ins, outs, flops, scratch=(), mib=16, space=pltpu.VMEM):
        return pl.pallas_call(
            body,
            out_shape=outs,
            in_specs=[pl.BlockSpec(memory_space=space)] * len(ins),
            out_specs=[pl.BlockSpec(memory_space=pltpu.VMEM)] * len(outs),
            scratch_shapes=list(scratch),
            compiler_params=params(mib),
            cost_estimate=cost(flops),
        )(*ins)

    def send(value, m, e):
        if not m and not e:
            return value
        if not e:
            return lax.ppermute(value, "dp", [(i, shift(i, m)) for i in range(dp)])
        if not m:
            return lax.ppermute(value, "cent", [(j, j ^ e) for j in range(cent)])
        pairs = [
            (i * cent + j, shift(i, m) * cent + (j ^ e)) for i in range(dp) for j in range(cent)
        ]
        return lax.ppermute(value, ("dp", "cent"), pairs)

    def exchange(value):
        return lax.all_to_all(value, ("dp", "cent"), 0, 0, tiled=True)

    table = owner_slot.reshape(-1, LANES)
    held = pltpu.VMEM((docs, width), jnp.bfloat16)
    first, tags, key = call(
        route,
        (assigned.reshape(1, docs), table, documents),
        [bf16(row_cap, width), i32(owners, 1, LANES), i32(8, docs)],
        2 * row_cap * docs * width,
        [
            pltpu.VMEM((1, docs), jnp.int32),
            pltpu.VMEM(table.shape, jnp.int32),
            held,
            pltpu.SemaphoreType.DMA((3,)),
        ],
        mib=62,
        space=pl.ANY,
    )
    tags = exchange(tags)
    got = call(
        pack,
        (key, documents),
        [bf16(row_cap, size(f)) for f in far[1:]]
        + [bf16(cap, width)] * (len(direct) * cent),
        2 * len(far) * row_cap * docs * width,
        [pltpu.VMEM((8, docs), jnp.int32), held, pltpu.SemaphoreType.DMA((2,))],
        mib=62,
        space=pl.ANY,
    )
    sent = {f: send(v, f[0], 0) for f, v in zip(far, [first, *got])}
    arrays = {}
    for n, m in enumerate(direct):
        near = got[len(far) - 1 + n * cent : len(far) - 1 + (n + 1) * cent]
        arrays[((m, 0, 4),)] = [send(v, m, e) for e, v in enumerate(near)]
    for part in relayed:
        wide = size(part[0])
        hop = call(
            make_relay(part),
            (tags, *[sent[f] for f in part]),
            [bf16(len(part) * cap, wide)] * cent,
            2 * len(part) * group * row_cap * wide,
        )
        arrays[part] = [send(hop[e], 0, e) for e in range(cent)]
    kept, cent_inv = call(norms, (centroids,), [bf16(rows, width), f32(rows, 1)], 2 * rows * width)
    olds, tally = [], None
    for s, parts in enumerate(stages):
        fresh = len(stage_masks(parts)) * group
        last = s == len(stages) - 1
        ins = [b for part in (parts[-1:] if last else parts) for b in arrays[part]]
        ins += [tags, kept, cent_inv]
        ins += [v for old in olds for v in old] + ([tally] if s else [])
        many = rows + fresh + sum(o[0].shape[0] for o in olds)
        flops = 2 * fresh * many * width
        if not last:
            outs = [bf16(fresh, width), f32(fresh, 2), f32(4, fresh), bf16(rows, fresh)]
            outs += [f32(rows, 3)] + [f32(*o[2].shape) for o in olds]
            x, col, line, own, tally, *lines = call(make_owner(s), ins, outs, flops)
            olds = [(o[0], o[1], l, o[3]) for o, l in zip(olds, lines)] + [(x, col, line, own)]
        else:
            early = [b for part in parts[:-1] for b in arrays[part]] + [kept] + [o[0] for o in olds]
            wide = span(parts[-1][0])[0]
            (acc,) = call(
                partial, early, [f32(many, fresh)], flops, [pltpu.VMEM((fresh, wide), jnp.bfloat16)]
            )
            scratch = [pltpu.VMEM((fresh, width - wide), jnp.bfloat16)]
            outs = [f32(owners, 1, 2 * cap), f32(3, rows)]
            scores, stats = call(make_owner(s), ins + [acc], outs, flops // 4, scratch)
    back = exchange(scores)
    outs = [f32(1, docs), f32(1, docs), f32(3, rows)]
    proto, red, stats = call(unpack, (back, key, stats), outs, 1 << 20)
    return proto.reshape(docs), red.reshape(docs), stats


def stage_masks(parts):
    out = []
    for part in parts:
        out += [f[0] for f in part if f[0] not in out]
    return out


def plan():
    whole = lambda *masks: tuple((m, 0, 4) for m in masks)
    cuts = [(5, 0, 2), (5, 2, 4)]
    far = [f[0] for f in map(whole, (4, 2, 6, 3, 7))] + cuts
    relayed = [(f,) for f in far]
    direct = [0, 1]
    stages = [
        [whole(0), whole(1)],
        [whole(4), whole(2), whole(6)],
        [whole(3), whole(7)],
        [(f,) for f in cuts],
    ]
    return far, direct, relayed, stages


def local_general(documents, assigned, centroids, owner_slot):
    doc_count, width = documents.shape
    table_rows = centroids.shape[0]
    dp_count = lax.axis_size("dp")
    cent_count = lax.axis_size("cent")
    owner_count = dp_count * cent_count
    pair_cap = 2 * doc_count // owner_count
    row_cap = 5 * cent_count * pair_cap // 8
    slot_ids = owner_slot[assigned]
    owner_ids = slot_ids // table_rows
    local_ids = slot_ids % table_rows
    row_ids = owner_ids // cent_count
    col_ids = owner_ids % cent_count
    first_pos = bucket_positions(row_ids, dp_count, row_cap)
    outgoing = jnp.zeros((dp_count * row_cap, width), jnp.bfloat16).at[first_pos].set(documents)
    tag_ids = (
        jnp.full((dp_count * row_cap,), -1, jnp.int32)
        .at[first_pos]
        .set(col_ids * table_rows + local_ids)
    )
    relayed, relayed_tags = (
        lax.all_to_all(
            outgoing.reshape(dp_count, row_cap, width),
            "dp",
            split_axis=0,
            concat_axis=0,
            tiled=True,
        ),
        lax.all_to_all(
            tag_ids.reshape(dp_count, row_cap), "dp", split_axis=0, concat_axis=0, tiled=True
        ),
    )
    relayed = relayed.reshape(-1, width)
    relayed_tags = relayed_tags.reshape(-1)
    relay_live = relayed_tags >= 0
    relay_target = jnp.where(relay_live, relayed_tags // table_rows, cent_count)
    inner_cap = dp_count * pair_cap
    second_pos = bucket_positions(relay_target, cent_count, inner_cap)
    forward = (
        jnp.zeros((cent_count * inner_cap, width), jnp.bfloat16)
        .at[second_pos]
        .set(relayed, mode="drop")
    )
    forward_tags = (
        jnp.full((cent_count * inner_cap,), -1, jnp.int32)
        .at[second_pos]
        .set(jnp.where(relay_live, relayed_tags % table_rows, -1), mode="drop")
    )
    incoming, incoming_tags = (
        lax.all_to_all(
            forward.reshape(cent_count, inner_cap, width),
            "cent",
            split_axis=0,
            concat_axis=0,
            tiled=True,
        ),
        lax.all_to_all(
            forward_tags.reshape(cent_count, inner_cap),
            "cent",
            split_axis=0,
            concat_axis=0,
            tiled=True,
        ),
    )
    cluster_totals, proto_score, redundant = owner_work(
        incoming.reshape(-1, width), incoming_tags.reshape(-1), centroids
    )
    back_score, back_redundant = (
        lax.all_to_all(
            proto_score.reshape(cent_count, inner_cap),
            "cent",
            split_axis=0,
            concat_axis=0,
            tiled=True,
        ),
        lax.all_to_all(
            redundant.reshape(cent_count, inner_cap),
            "cent",
            split_axis=0,
            concat_axis=0,
            tiled=True,
        ),
    )
    safe_pos = jnp.clip(second_pos, 0, cent_count * inner_cap - 1)
    relay_score = jnp.where(relay_live, back_score.reshape(-1)[safe_pos], 0.0)
    relay_redundant = jnp.where(relay_live, back_redundant.reshape(-1)[safe_pos], 0.0)
    home_score, home_redundant = (
        lax.all_to_all(
            relay_score.reshape(dp_count, row_cap), "dp", split_axis=0, concat_axis=0, tiled=True
        ),
        lax.all_to_all(
            relay_redundant.reshape(dp_count, row_cap),
            "dp",
            split_axis=0,
            concat_axis=0,
            tiled=True,
        ),
    )
    prototypicality = home_score.reshape(-1)[first_pos]
    redundancy = home_redundant.reshape(-1)[first_pos]
    return (prototypicality, redundancy, cluster_totals)


def solution(mesh):
    in_specs = (P(("dp", "cent"), None), P(("dp", "cent")), P(("dp", "cent"), None), P())
    out_specs = (P(("dp", "cent")), P(("dp", "cent")), P(None, ("dp", "cent")))
    dp, cent = mesh.shape["dp"], mesh.shape["cent"]
    small = dp == 8 and cent & (cent - 1) == 0

    def body(*args):
        return (local if small else local_general)(*args)

    return jax.shard_map(body, mesh=mesh, in_specs=in_specs, out_specs=out_specs, check_vma=False)
```

```python
import math

import jax
import jax.numpy as jnp
from jax import lax
from jax.experimental import pallas as pl
from jax.experimental.pallas import tpu as pltpu
from jax.sharding import PartitionSpec as P


LANES = 128
HIGHEST = lax.Precision.HIGHEST


def bucket_positions(target, groups, capacity):
    length = target.shape[0]
    indicator = (target[:, None] == jnp.arange(groups, dtype=jnp.int32)[None, :]).astype(
        jnp.bfloat16
    )
    earlier = (
        lax.broadcasted_iota(jnp.int32, (length, length), 0)
        > lax.broadcasted_iota(jnp.int32, (length, length), 1)
    ).astype(jnp.bfloat16)
    before = jnp.dot(earlier, indicator, preferred_element_type=jnp.float32)
    rank_ids = jnp.sum(before * indicator.astype(jnp.float32), axis=1).astype(jnp.int32)
    return jnp.where(target < groups, target * capacity + rank_ids, groups * capacity)


def owner_work(incoming, incoming_tags, centroids):
    table_rows = centroids.shape[0]
    width = incoming.shape[1]
    length = incoming_tags.shape[0]
    is_live = incoming_tags >= 0
    safe_slot = jnp.clip(incoming_tags, 0, table_rows - 1)
    cent_sq = jnp.einsum("kd,kd->k", centroids, centroids, preferred_element_type=jnp.float32)
    cent_vec = centroids[safe_slot]
    cross_dot = jnp.einsum("sd,sd->s", incoming, cent_vec, preferred_element_type=jnp.float32)
    self_sq = jnp.einsum("sd,sd->s", incoming, incoming, preferred_element_type=jnp.float32)
    inverse_norm = lax.rsqrt(self_sq + 1.0)
    similarity = cross_dot * inverse_norm * lax.rsqrt(cent_sq[safe_slot] + 1.0)
    members = (incoming_tags[:, None] == jnp.arange(table_rows, dtype=jnp.int32)[None, :]).astype(
        jnp.float32
    )
    live_weight = is_live.astype(jnp.float32)
    moments = jnp.stack(
        [live_weight, live_weight * similarity, live_weight * similarity * similarity]
    )
    cluster_totals = jnp.dot(
        moments, members, precision=lax.Precision.HIGHEST, preferred_element_type=jnp.float32
    )
    count_floor = jnp.maximum(cluster_totals[0], 1.0)
    mean_sim = cluster_totals[1] / count_floor
    variance = jnp.maximum(cluster_totals[2] / count_floor - mean_sim * mean_sim, 0.0)
    proto_score = jnp.where(
        is_live,
        (mean_sim[safe_slot] - similarity) / jnp.sqrt(variance[safe_slot] + 1.0 / width),
        0.0,
    )
    gram_block = lax.dot_general(
        incoming, incoming, (((1,), (1,)), ((), ())), preferred_element_type=jnp.float32
    )
    cosine = gram_block * inverse_norm[:, None] * inverse_norm[None, :]
    not_self = lax.broadcasted_iota(jnp.int32, (length, length), 0) != lax.broadcasted_iota(
        jnp.int32, (length, length), 1
    )
    same_cluster = (incoming_tags[:, None] == incoming_tags[None, :]) & is_live[:, None] & not_self
    redundant = math.sqrt(width) * jnp.max(jnp.where(same_cluster, cosine, 0.0), axis=1)
    return (cluster_totals, proto_score, redundant)


def iota(shape, dim):
    return lax.broadcasted_iota(jnp.int32, shape, dim)


def mm(a, b, dims, precision=None):
    return lax.dot_general(
        a, b, (dims, ((), ())), precision=precision, preferred_element_type=jnp.float32
    )


def ring(dp):
    line = dp >> 1
    return line ^ (line >> 1)


def shift(dp, m):
    place = (ring(dp) + (m >> 1)) & 3
    return ((place ^ (place >> 1)) << 1) | ((dp ^ m) & 1)


def back_shift(dp, m):
    return shift(dp, ((8 - (m & 6)) & 6) | (m & 1))


def relative(owner_dp, dp):
    return (((ring(owner_dp) - ring(dp)) & 3) << 1) | ((owner_dp ^ dp) & 1)


def params(mib):
    return pltpu.CompilerParams(vmem_limit_bytes=mib * 1024 * 1024)


def local(documents, assigned, centroids, owner_slot):
    docs, width = documents.shape
    rows = centroids.shape[0]
    dp = lax.axis_size("dp")
    cent = lax.axis_size("cent")
    owners = dp * cent
    cap = 2 * docs // owners
    row_cap = 5 * cent * cap // 8
    group = cent * cap
    clusters = owner_slot.shape[0]
    root = math.sqrt(width)
    far, direct, relayed, stages = plan()
    source = lambda m, e: back_shift(lax.axis_index("dp"), m) * cent + (lax.axis_index("cent") ^ e)
    span = lambda f: (f[1] * width // 8, f[2] * width // 8)
    size = lambda f: span(f)[1] - span(f)[0]

    def route(assigned_hbm, table_hbm, docs_hbm, far_ref, tag_ref, key_ref, *scratch):
        assigned_ref, table_ref, docs_ref, sems = scratch
        copies = [
            pltpu.make_async_copy(src, dst, sems.at[n])
            for n, (src, dst) in enumerate(
                [(assigned_hbm, assigned_ref), (table_hbm, table_ref), (docs_hbm, docs_ref)]
            )
        ]
        for copy in copies:
            copy.start()
        copies[0].wait()
        copies[1].wait()
        a = assigned_ref[...]
        pick = (iota((clusters // LANES, docs), 0) == a // LANES).astype(jnp.bfloat16)
        digits, left = [], clusters - 1
        while left:
            digits.append((table_ref[...] >> (7 * len(digits))) & (LANES - 1))
            left >>= 7
        digits = [d.astype(jnp.float32).astype(jnp.bfloat16) for d in digits]
        lines = mm(jnp.concatenate(digits, axis=1), pick, ((0,), (0,)))
        value = lines[:LANES]
        for n in range(1, len(digits)):
            value = value + lines[n * LANES : (n + 1) * LANES] * float(LANES**n)
        slot = jnp.sum(
            jnp.where(iota((LANES, docs), 0) == a % LANES, value, 0.0), axis=0, keepdims=True
        )
        owner = jnp.floor((slot + 0.5) * (1.0 / rows))
        home = (slot - owner * rows).astype(jnp.int32) + 1
        owner = owner.astype(jnp.int32)
        here, side = lax.axis_index("dp"), lax.axis_index("cent")
        rel = relative(owner // cent, here) * cent + ((owner % cent) ^ side)
        which = iota((owners, docs), 0)
        mine = which == owner
        near = which // cent == owner // cent
        earlier = (iota((LANES, LANES), 0) < iota((LANES, LANES), 1)).astype(jnp.bfloat16)
        marks = mine.astype(jnp.float32)
        before, total = [], jnp.zeros((owners, 1), jnp.float32)
        for lo in range(0, docs, LANES):
            part = marks[:, lo : lo + LANES]
            before.append(mm(part.astype(jnp.bfloat16), earlier, ((1,), (0,))) + total)
            total = total + jnp.sum(part, axis=1, keepdims=True)
        before = jnp.concatenate(before, axis=1)
        count = lambda m: jnp.sum(jnp.where(m, before, 0.0), axis=0, keepdims=True)
        rank = count(mine).astype(jnp.int32)
        row_rank = count(near).astype(jnp.int32)
        key = rel * cap + rank
        row_key = (rel // cent) * row_cap + row_rank
        key_ref[0:1, :] = key
        key_ref[1:2, :] = row_key
        key_ref[2:3, :] = owner
        spread = lambda m, v: jnp.where(m, v.astype(jnp.float32), 0.0).astype(jnp.bfloat16)
        at_rank = (iota((cap, docs), 0) == rank).astype(jnp.bfloat16)
        at_row = (iota((row_cap, docs), 0) == row_rank).astype(jnp.bfloat16)
        homes = jnp.concatenate([spread(mine, home // LANES), spread(mine, home % LANES)], axis=0)
        homes = mm(homes, at_rank, ((1,), (1,)))
        homes = homes[:owners] * float(LANES) + homes[owners:]
        inners = mm(spread(near, key % group + 1), at_row, ((1,), (1,)))
        tag_ref[...] = jnp.zeros((owners, 1, LANES), jnp.int32)
        tag_ref[:, 0, :cap] = homes.astype(jnp.int32)
        tag_ref[:, 0, cap : cap + row_cap] = inners.astype(jnp.int32)
        sel = iota((row_cap, docs), 0) + far[0][0] * row_cap == row_key
        copies[2].wait()
        picked = mm(sel.astype(jnp.bfloat16), docs_ref[...], ((1,), (0,)))
        far_ref[...] = picked.astype(jnp.bfloat16)

    def pack(key_hbm, docs_hbm, *refs):
        *outs, key_ref, docs_ref, sems = refs
        copies = [
            pltpu.make_async_copy(key_hbm, key_ref, sems.at[0]),
            pltpu.make_async_copy(docs_hbm, docs_ref, sems.at[1]),
        ]
        for copy in copies:
            copy.start()
        copies[0].wait()
        key, row_key = key_ref[0:1, :], key_ref[1:2, :]
        rest = sorted({f[0] for f in far[1:]})
        sel = [iota((row_cap, docs), 0) + m * row_cap == row_key for m in rest]
        ahead = stages[-1][-1][0]
        sel += [iota((group, docs), 0) + m * group == key for m in direct + [ahead[0]]]
        sel = jnp.concatenate([v.astype(jnp.bfloat16) for v in sel], axis=0)
        copies[1].wait()
        step = width // 8
        for lo in range(0, width, step):
            picked = mm(sel, docs_ref[:, lo : lo + step], ((1,), (0,))).astype(jnp.bfloat16)
            for ref, f in zip(outs, far[1:]):
                at = rest.index(f[0]) * row_cap
                if span(f)[0] <= lo < span(f)[1]:
                    lane = lo - span(f)[0]
                    ref[:, lane : lane + step] = picked[at : at + row_cap]
            for n, ref in enumerate(outs[len(far) - 1 :]):
                at = len(rest) * row_cap + n * cap
                if n < len(direct) * cent:
                    ref[:, lo : lo + step] = picked[at : at + cap]
                elif span(ahead)[0] <= lo < span(ahead)[1]:
                    lane = lo - span(ahead)[0]
                    ref[:, lane : lane + step] = picked[at : at + cap]

    def join(*refs):
        for n, ref in enumerate(refs[:-1]):
            refs[-1][n * cap : (n + 1) * cap, :] = ref[...]

    def norms(cent_ref, keep_ref, inv_ref):
        keep_ref[...] = cent_ref[...]
        c = cent_ref[...].astype(jnp.float32)
        inv_ref[...] = lax.rsqrt(jnp.sum(c * c, axis=1, keepdims=True) + 1.0)

    def make_relay(part):
        def body(tag_ref, *refs):
            for n, (m, _, _) in enumerate(part):
                tags = tag_ref[pl.ds(source(m, 0), 1), 0, cap : cap + row_cap]
                sel = (iota((group, row_cap), 0) + 1 == tags).astype(jnp.bfloat16)
                picked = mm(sel, refs[n][...], ((1,), (0,))).astype(jnp.bfloat16)
                for e in range(cent):
                    refs[len(part) + e][n * cap : (n + 1) * cap] = picked[e * cap : (e + 1) * cap]

        return body

    def fill(x, parts, masks, arrays):
        start = span(parts[0][0])[0] if len(masks) == 1 else 0
        for part, refs in zip(parts, arrays):
            for i, f in enumerate(part):
                lo, hi = span(f)
                for e in range(cent):
                    at = (masks.index(f[0]) * cent + e) * cap
                    x[at : at + cap, lo - start : hi - start] = refs[e][i * cap : (i + 1) * cap, :]

    def partial(*refs):
        parts = stages[-1][:-1]
        refs = list(refs)
        arrays = [[refs.pop(0) for _ in range(cent)] for _ in parts]
        *lefts, acc_ref, x = refs
        fill(x, parts, stage_masks(parts), arrays)
        xn, base = x[...], 0
        for left in lefts:
            out = mm(left[:, : xn.shape[1]], xn, ((1,), (1,)))
            acc_ref[base : base + out.shape[0], :] = out
            base += out.shape[0]
        acc_ref[base:, :] = mm(xn, xn, ((1,), (1,)))

    def make_owner(s):
        parts = stages[s]
        masks = stage_masks(parts)
        fresh = len(masks) * group
        last = s == len(stages) - 1

        def body(*refs):
            refs = list(refs)
            take = lambda n: [refs.pop(0) for _ in range(n)]
            arrays = [take(1)] if last else [take(cent) for _ in parts]
            tag_ref, cent_ref, cent_inv_ref = take(3)
            olds = [take(4) for _ in range(s)]
            tally = take(1)[0] if s else None
            acc_ref = take(1)[0] if last else None
            if last:
                score_ref, stat_ref = take(2)
            else:
                x, col, line, own_ref, tally_out = take(5)
                old_outs = take(s)
            if not last:
                fill(x, parts, masks, arrays)
            lane = slice(*span(parts[-1][0])) if last else slice(None)
            base = [0]

            def dots(left, right):
                out = mm(left[:, lane], right, ((1,), (1,)))
                if last:
                    out = out + acc_ref[base[0] : base[0] + out.shape[0], :]
                base[0] += out.shape[0]
                return out

            tags = [
                tag_ref[pl.ds(source(m, e), 1), 0, :cap] for m in masks for e in range(cent)
            ]
            tag = jnp.concatenate(tags, axis=1).astype(jnp.float32)
            eye = iota((LANES, LANES), 0) == iota((LANES, LANES), 1)

            def to_row(v):
                pieces = [
                    jnp.sum(jnp.where(eye, v[i : i + LANES], 0.0), axis=0, keepdims=True)
                    for i in range(0, v.shape[0], LANES)
                ]
                return jnp.concatenate(pieces, axis=1) if len(pieces) > 1 else pieces[0]

            def to_col(v):
                pieces = [
                    jnp.sum(jnp.where(eye, v[:, i : i + LANES], 0.0), axis=1, keepdims=True)
                    for i in range(0, v.shape[1], LANES)
                ]
                return jnp.concatenate(pieces, axis=0) if len(pieces) > 1 else pieces[0]

            cent_inv = cent_inv_ref[...]
            if s == 0:
                counts = [jnp.zeros((rows, 1), jnp.float32)] * 3
            else:
                counts = [tally[:, i : i + 1] for i in range(3)]
            xn = arrays[0][0][...] if last else x[...]
            cross = dots(cent_ref, xn)
            grams = [dots(old[0], xn) for old in olds]
            own_gram = mm(xn, xn, ((1,), (1,))) + (acc_ref[base[0] :, :] if last else 0.0)
            cols, lines = [], []
            for i in range(0, fresh, LANES):
                diag = jnp.where(eye, own_gram[i : i + LANES, i : i + LANES], 0.0)
                cols.append(lax.rsqrt(jnp.sum(diag, axis=1, keepdims=True) + 1.0))
                lines.append(lax.rsqrt(jnp.sum(diag, axis=0, keepdims=True) + 1.0))
            tag_col = to_col(tag)
            inv_col = jnp.concatenate(cols, axis=0)
            inv = jnp.concatenate(lines, axis=1)
            own = (iota((rows, fresh), 0) + 1).astype(jnp.float32) == tag
            sim = jnp.sum(jnp.where(own, cross * cent_inv, 0.0), axis=0, keepdims=True) * inv
            add = lambda v: jnp.sum(jnp.where(own, v, 0.0), axis=1, keepdims=True)
            counts = [c + add(v) for c, v in zip(counts, (jnp.ones_like(sim), sim, sim * sim))]
            same = (tag_col == tag) & (iota((fresh, fresh), 0) != iota((fresh, fresh), 1))
            best = jnp.max(jnp.where(same, own_gram * inv_col, 0.0), axis=0, keepdims=True)
            old_best = []
            for gram, (_, col_old, line_old, _) in zip(grams, olds):
                same = col_old[:, 0:1] == tag
                up = jnp.max(
                    jnp.where(same, gram * col_old[:, 1:2], 0.0), axis=0, keepdims=True
                )
                best = jnp.maximum(best, up)
                down = jnp.max(jnp.where(same, gram * inv, 0.0), axis=1, keepdims=True)
                old_best.append(jnp.maximum(line_old[3:4, :], to_row(down)))
            if not last:
                col[:, 0:1] = tag_col
                col[:, 1:2] = inv_col
                for i, v in enumerate((tag, inv, sim, best)):
                    line[i : i + 1, :] = v
                for i, v in enumerate(counts):
                    tally_out[:, i : i + 1] = v
                own_ref[...] = own.astype(jnp.bfloat16)
                for ref, (_, _, line_old, _), v in zip(old_outs, olds, old_best):
                    ref[0:3, :] = line_old[0:3, :]
                    ref[3:4, :] = v
                return
            count, s1, s2 = [to_row(v) for v in counts]
            for i, v in enumerate((count, s1, s2)):
                stat_ref[i : i + 1, :] = v
            floor = jnp.maximum(count, 1.0)
            mean = s1 / floor
            var = jnp.maximum(s2 / floor - mean * mean, 0.0)
            terms = []
            for v in (mean, 1.0 / jnp.sqrt(var + 1.0 / width)):
                for _ in range(3):
                    terms.append(v.astype(jnp.bfloat16).astype(jnp.float32))
                    v = v - terms[-1]
            table = jnp.zeros((8, rows), jnp.float32)
            for i, v in enumerate(terms):
                table = jnp.where(iota((8, rows), 0) == i, v, table)
            table = table.astype(jnp.bfloat16)
            facts = [(l[1:2, :], l[2:3, :], v, o) for (_, _, l, o), v in zip(olds, old_best)]
            facts.append((inv, sim, best, own.astype(jnp.bfloat16)))
            for parts_s, (inv, sim, best, own) in zip(stages, facts):
                order_s = stage_masks(parts_s)
                got = mm(table, own[...], ((1,), (0,)))
                mean_d = got[0:1, :] + got[1:2, :] + got[2:3, :]
                spread_d = got[3:4, :] + got[4:5, :] + got[5:6, :]
                score = (mean_d - sim) * spread_d
                red = best * inv * root
                for b in range(len(order_s) * cent):
                    part = slice(b * cap, (b + 1) * cap)
                    score_ref[pl.ds(source(order_s[b // cent], b % cent), 1), 0, :] = jnp.concatenate(
                        [score[:, part], red[:, part]], axis=1
                    )

        return body

    def unpack(score_ref, key_ref, stat_ref, out_ref, red_ref, stat_out):
        stat_out[...] = stat_ref[...]
        key = key_ref[0:1, :]
        pick = (iota((owners, docs), 0) == key_ref[2:3, :]).astype(jnp.float32)
        got = mm(score_ref[:, 0, :], pick, ((0,), (0,)), HIGHEST)
        rank = iota((2 * cap, docs), 0)
        out_ref[...] = jnp.sum(jnp.where(rank == key % cap, got, 0.0), axis=0, keepdims=True)
        red_ref[...] = jnp.sum(jnp.where(rank == key % cap + cap, got, 0.0), axis=0, keepdims=True)

    f32 = lambda *s: jax.ShapeDtypeStruct(s, jnp.float32)
    bf16 = lambda *s: jax.ShapeDtypeStruct(s, jnp.bfloat16)
    i32 = lambda *s: jax.ShapeDtypeStruct(s, jnp.int32)
    cost = lambda n: pl.CostEstimate(flops=n, bytes_accessed=1 << 20, transcendentals=0)

    def call(body, ins, outs, flops, scratch=(), mib=16, space=pltpu.VMEM):
        return pl.pallas_call(
            body,
            out_shape=outs,
            in_specs=[pl.BlockSpec(memory_space=space)] * len(ins),
            out_specs=[pl.BlockSpec(memory_space=pltpu.VMEM)] * len(outs),
            scratch_shapes=list(scratch),
            compiler_params=params(mib),
            cost_estimate=cost(flops),
        )(*ins)

    def send(value, m, e):
        if not m and not e:
            return value
        if not e:
            return lax.ppermute(value, "dp", [(i, shift(i, m)) for i in range(dp)])
        if not m:
            return lax.ppermute(value, "cent", [(j, j ^ e) for j in range(cent)])
        pairs = [
            (i * cent + j, shift(i, m) * cent + (j ^ e)) for i in range(dp) for j in range(cent)
        ]
        return lax.ppermute(value, ("dp", "cent"), pairs)

    def exchange(value):
        return lax.all_to_all(value, ("dp", "cent"), 0, 0, tiled=True)

    table = owner_slot.reshape(-1, LANES)
    held = pltpu.VMEM((docs, width), jnp.bfloat16)
    first, tags, key = call(
        route,
        (assigned.reshape(1, docs), table, documents),
        [bf16(row_cap, width), i32(owners, 1, LANES), i32(8, docs)],
        2 * row_cap * docs * width,
        [
            pltpu.VMEM((1, docs), jnp.int32),
            pltpu.VMEM(table.shape, jnp.int32),
            held,
            pltpu.SemaphoreType.DMA((3,)),
        ],
        mib=62,
        space=pl.ANY,
    )
    tags = exchange(tags)
    got = call(
        pack,
        (key, documents),
        [bf16(row_cap, size(f)) for f in far[1:]]
        + [bf16(cap, width)] * (len(direct) * cent)
        + [bf16(cap, size(stages[-1][-1][0]))] * cent,
        2 * len(far) * row_cap * docs * width,
        [pltpu.VMEM((8, docs), jnp.int32), held, pltpu.SemaphoreType.DMA((2,))],
        mib=62,
        space=pl.ANY,
    )
    sent = {f: send(v, f[0], 0) for f, v in zip(far, [first, *got])}
    arrays = {}
    for n, m in enumerate(direct):
        near = got[len(far) - 1 + n * cent : len(far) - 1 + (n + 1) * cent]
        arrays[((m, 0, 8),)] = [send(v, m, e) for e, v in enumerate(near)]
    for part in relayed:
        wide = size(part[0])
        hop = call(
            make_relay(part),
            (tags, *[sent[f] for f in part]),
            [bf16(len(part) * cap, wide)] * cent,
            2 * len(part) * group * row_cap * wide,
        )
        arrays[part] = [send(hop[e], 0, e) for e in range(cent)]
    kept, cent_inv = call(norms, (centroids,), [bf16(rows, width), f32(rows, 1)], 2 * rows * width)
    ahead = stages[-1][-1][0]
    early = got[len(far) - 1 + len(direct) * cent :]
    early = [send(v, 0, e) for e, v in enumerate(early)]
    (joined,) = call(join, early, [bf16(group, size(ahead))], 1 << 10)
    arrays[(ahead,)] = [send(joined, ahead[0], 0)]
    olds, tally = [], None
    for s, parts in enumerate(stages):
        fresh = len(stage_masks(parts)) * group
        last = s == len(stages) - 1
        ins = [b for part in (parts[-1:] if last else parts) for b in arrays[part]]
        ins += [tags, kept, cent_inv]
        ins += [v for old in olds for v in old] + ([tally] if s else [])
        many = rows + fresh + sum(o[0].shape[0] for o in olds)
        flops = 2 * fresh * many * width
        if not last:
            outs = [bf16(fresh, width), f32(fresh, 2), f32(4, fresh), bf16(rows, fresh)]
            outs += [f32(rows, 3)] + [f32(*o[2].shape) for o in olds]
            x, col, line, own, tally, *lines = call(make_owner(s), ins, outs, flops)
            olds = [(o[0], o[1], l, o[3]) for o, l in zip(olds, lines)] + [(x, col, line, own)]
        else:
            early = [b for part in parts[:-1] for b in arrays[part]] + [kept] + [o[0] for o in olds]
            wide = span(parts[-1][0])[0]
            (acc,) = call(
                partial, early, [f32(many, fresh)], flops, [pltpu.VMEM((fresh, wide), jnp.bfloat16)]
            )
            outs = [f32(owners, 1, 2 * cap), f32(3, rows)]
            scores, stats = call(make_owner(s), ins + [acc], outs, flops // 4)
    back = exchange(scores)
    outs = [f32(1, docs), f32(1, docs), f32(3, rows)]
    proto, red, stats = call(unpack, (back, key, stats), outs, 1 << 20)
    return proto.reshape(docs), red.reshape(docs), stats


def stage_masks(parts):
    out = []
    for part in parts:
        out += [f[0] for f in part if f[0] not in out]
    return out


def plan():
    whole = lambda *masks: tuple((m, 0, 8) for m in masks)
    cuts = [(5, 0, 5), (5, 5, 8)]
    far = [f[0] for f in map(whole, (4, 2, 6, 3, 7))] + cuts[:1]
    relayed = [(f,) for f in far]
    direct = [0, 1]
    stages = [
        [whole(0), whole(1)],
        [whole(4), whole(2), whole(6)],
        [whole(3), whole(7)],
        [(f,) for f in cuts],
    ]
    return far, direct, relayed, stages


def local_general(documents, assigned, centroids, owner_slot):
    doc_count, width = documents.shape
    table_rows = centroids.shape[0]
    dp_count = lax.axis_size("dp")
    cent_count = lax.axis_size("cent")
    owner_count = dp_count * cent_count
    pair_cap = 2 * doc_count // owner_count
    row_cap = 5 * cent_count * pair_cap // 8
    slot_ids = owner_slot[assigned]
    owner_ids = slot_ids // table_rows
    local_ids = slot_ids % table_rows
    row_ids = owner_ids // cent_count
    col_ids = owner_ids % cent_count
    first_pos = bucket_positions(row_ids, dp_count, row_cap)
    outgoing = jnp.zeros((dp_count * row_cap, width), jnp.bfloat16).at[first_pos].set(documents)
    tag_ids = (
        jnp.full((dp_count * row_cap,), -1, jnp.int32)
        .at[first_pos]
        .set(col_ids * table_rows + local_ids)
    )
    relayed, relayed_tags = (
        lax.all_to_all(
            outgoing.reshape(dp_count, row_cap, width),
            "dp",
            split_axis=0,
            concat_axis=0,
            tiled=True,
        ),
        lax.all_to_all(
            tag_ids.reshape(dp_count, row_cap), "dp", split_axis=0, concat_axis=0, tiled=True
        ),
    )
    relayed = relayed.reshape(-1, width)
    relayed_tags = relayed_tags.reshape(-1)
    relay_live = relayed_tags >= 0
    relay_target = jnp.where(relay_live, relayed_tags // table_rows, cent_count)
    inner_cap = dp_count * pair_cap
    second_pos = bucket_positions(relay_target, cent_count, inner_cap)
    forward = (
        jnp.zeros((cent_count * inner_cap, width), jnp.bfloat16)
        .at[second_pos]
        .set(relayed, mode="drop")
    )
    forward_tags = (
        jnp.full((cent_count * inner_cap,), -1, jnp.int32)
        .at[second_pos]
        .set(jnp.where(relay_live, relayed_tags % table_rows, -1), mode="drop")
    )
    incoming, incoming_tags = (
        lax.all_to_all(
            forward.reshape(cent_count, inner_cap, width),
            "cent",
            split_axis=0,
            concat_axis=0,
            tiled=True,
        ),
        lax.all_to_all(
            forward_tags.reshape(cent_count, inner_cap),
            "cent",
            split_axis=0,
            concat_axis=0,
            tiled=True,
        ),
    )
    cluster_totals, proto_score, redundant = owner_work(
        incoming.reshape(-1, width), incoming_tags.reshape(-1), centroids
    )
    back_score, back_redundant = (
        lax.all_to_all(
            proto_score.reshape(cent_count, inner_cap),
            "cent",
            split_axis=0,
            concat_axis=0,
            tiled=True,
        ),
        lax.all_to_all(
            redundant.reshape(cent_count, inner_cap),
            "cent",
            split_axis=0,
            concat_axis=0,
            tiled=True,
        ),
    )
    safe_pos = jnp.clip(second_pos, 0, cent_count * inner_cap - 1)
    relay_score = jnp.where(relay_live, back_score.reshape(-1)[safe_pos], 0.0)
    relay_redundant = jnp.where(relay_live, back_redundant.reshape(-1)[safe_pos], 0.0)
    home_score, home_redundant = (
        lax.all_to_all(
            relay_score.reshape(dp_count, row_cap), "dp", split_axis=0, concat_axis=0, tiled=True
        ),
        lax.all_to_all(
            relay_redundant.reshape(dp_count, row_cap),
            "dp",
            split_axis=0,
            concat_axis=0,
            tiled=True,
        ),
    )
    prototypicality = home_score.reshape(-1)[first_pos]
    redundancy = home_redundant.reshape(-1)[first_pos]
    return (prototypicality, redundancy, cluster_totals)


def solution(mesh):
    in_specs = (P(("dp", "cent"), None), P(("dp", "cent")), P(("dp", "cent"), None), P())
    out_specs = (P(("dp", "cent")), P(("dp", "cent")), P(None, ("dp", "cent")))
    dp, cent = mesh.shape["dp"], mesh.shape["cent"]
    small = dp == 8 and cent & (cent - 1) == 0

    def body(*args):
        return (local if small else local_general)(*args)

    return jax.shard_map(body, mesh=mesh, in_specs=in_specs, out_specs=out_specs, check_vma=False)
```
